32 devices in a mesh: chan: 4 (over z), tm: 8 (over y, x, core).
Axes of the slice: x: 2, y: 2, z: 4, core: 2. Of those that a mesh axis runs over, the one named last changes fastest.
Arguments:
- voltages: bfloat16 [2, 64, 4, 524288], P(None, 'tm', 'chan'), may hold values from -6 to 6
- antenna_gains: float32 [2, 64, 4], P(None, None, 'chan'), may hold values from -0.75 to 0.75
- chirp_phase: float32 [4, 131072], P('chan'), may hold values from -3.140625 to 3.140625
- offsets: int32 [4], P('chan'), may hold values from 0 to 4095, as said below
- flags: int32 [4, 512], P('chan', 'tm'), may hold values 0 or 1
- sample_phase_bins: int32 [524288], P('tm'), may hold values from 0 to 2047
Outputs:
- dedispersed: bfloat16 [2, 4, 524288], P(None, 'chan', 'tm')
- sk_weight: float32 [4, 512], P('chan', 'tm')
- profile: float32 [4, 2048], P('chan', 'tm')
- band_profile: float32 [2048], P('tm')
The draws below stay inside these ranges and needn't reach their ends.
Inputs may be any that keep to these rules, and one draw needn't show every extreme that they name: `offsets`: some channel has the offset 4096 - 1.
All inputs are finite; a program needn't handle non-finite values. No bound on the sum of `flags` on one device may be relied on, other than what follows from the above.
Results may differ from the reference program's by a relative error of at most 0.0045.
Values may be sent and summed in bfloat16 or wider, within the bound.
A program may use at most 192 MiB of HBM per device.

```python
import jax
import jax.numpy as jnp
from jax import lax

ANTENNA_COUNT = 64
NFFT = 131072
OFFSET_BOUND = 4096
SKW = 1024
BINS = 2048
TS = 65536
CHANNEL_COUNT = 4
TIME_SAMPLES = 524288
NWIN = 512
N_TM = 8


def draw_offsets(key, part):
    values = jax.random.randint(jax.random.fold_in(key, 11), (CHANNEL_COUNT,), 0, OFFSET_BOUND, dtype=jnp.int32)
    chosen = jax.random.randint(jax.random.fold_in(key, 12), (), 0, CHANNEL_COUNT, dtype=jnp.int32)
    marker = jnp.arange(CHANNEL_COUNT, dtype=jnp.int32) == chosen
    return jnp.where(marker, OFFSET_BOUND - 1, values).astype(jnp.int32)


def place_ends(array, key, smallest, top_value):
    extent = array.shape
    spot = [jax.random.randint(jax.random.fold_in(key, axis), (), 0, extent[axis]) for axis in range(len(extent))]
    array = array.at[tuple(spot)].set(smallest)
    longest = extent.index(max(extent))
    spot[longest] = (spot[longest] + 1) % extent[longest]
    return array.at[tuple(spot)].set(top_value)


def with_spikes(drawn, rng, source, target, blocks, factor):
    def block_of(dim):
        return (jnp.arange(drawn.shape[dim]) // (drawn.shape[dim] // blocks)).reshape((-1,) + (1,) * (drawn.ndim - 1 - dim))

    near = jax.random.permutation(rng, blocks)[block_of(target)]
    far = (block_of(target) + blocks // 2) % blocks
    return jnp.where((block_of(source) == near) | (block_of(source) == far), factor * drawn, drawn)


def steps_of(rng, shape, shards, smallest, top_value):
    level, own = 1.0, jax.random.fold_in(rng, 6)
    for axis_at, parts in shards:
        draws = jnp.exp(jax.random.uniform(jax.random.fold_in(own, axis_at), (parts,), jnp.float32, smallest / len(shards), top_value / len(shards)))
        level = level * jnp.repeat(draws, shape[axis_at] // parts).reshape([-1 if axis == axis_at else 1 for axis in range(len(shape))])
    return level


def scatter_about(key, extent, scale, reach, shards=(), held_as=jnp.bfloat16):
    level = steps_of(key, extent, shards, -0.22, 0.18) if shards else 1.0
    values = jax.random.normal(key, extent, jnp.float32) * scale * level
    return jnp.minimum(jnp.maximum(values, -reach), reach).astype(held_as)


def heavy_noise(own_key, extent, spread, bound, pieces, heavy, held_as=jnp.bfloat16):
    entries = spread * jax.random.normal(own_key, extent, jnp.float32)
    if pieces:
        entries = entries * steps_of(own_key, extent, pieces, -0.22, 0.18)
    return jnp.clip(with_spikes(entries, jax.random.fold_in(own_key, 3), *heavy), -bound, bound).astype(held_as)


def setup_inputs(seed: int = 0) -> dict:
    seeds = jax.random.split(jax.random.key(seed), 7)
    voltages = heavy_noise(seeds[0], (2, ANTENNA_COUNT, CHANNEL_COUNT, TIME_SAMPLES), 1.0, 6.0, ((1, 8), (2, 4)), (1, 3, 8, 2.0))
    antenna_gains = scatter_about(seeds[1], (2, ANTENNA_COUNT, CHANNEL_COUNT), ANTENNA_COUNT ** -0.5, 0.75, ((2, 4),), jnp.float32)
    chirp_phase = jnp.clip(jax.random.uniform(seeds[2], (CHANNEL_COUNT, NFFT), jnp.float32, -3.140625, 3.140625), -3.140625, 3.140625)
    offsets = draw_offsets(jax.random.fold_in(seeds[6], 71), 0)
    flags = place_ends((jax.random.randint(seeds[4], (CHANNEL_COUNT, NWIN), 0, 8) < 1).astype(jnp.int32), jax.random.fold_in(seeds[4], 1), 0, 1)
    sample_phase_bins = place_ends(jax.random.randint(seeds[5], (TIME_SAMPLES,), 0, BINS), jax.random.fold_in(seeds[5], 1), 0, BINS - 1).astype(jnp.int32)
    return {"voltages": voltages, "antenna_gains": antenna_gains, "chirp_phase": chirp_phase, "offsets": offsets, "flags": flags, "sample_phase_bins": sample_phase_bins}


SK_WIDTH = 0.05
EPSILON = 1e-6


def reference(voltages, antenna_gains, chirp_phase, offsets, flags, sample_phase_bins):
    def beam_channel(channel):
        samples = lax.dynamic_index_in_dim(voltages, channel, 2, keepdims=False).astype(jnp.float32)
        weights = lax.dynamic_index_in_dim(antenna_gains, channel, 2, keepdims=False)
        weight_real = weights[0][:, None]
        weight_imag = weights[1][:, None]
        out_real = jnp.sum(weight_real * samples[0] - weight_imag * samples[1], axis=0)
        out_imag = jnp.sum(weight_real * samples[1] + weight_imag * samples[0], axis=0)
        return jnp.stack([out_real, out_imag])

    beam_sum = lax.map(beam_channel, jnp.arange(CHANNEL_COUNT, dtype=jnp.int32))

    def dedisperse_channel(items):
        beam_pair, phase_row, start_at = items
        padded = jnp.pad(beam_pair, ((0, 0), (TS, TS)))
        shifted = lax.dynamic_slice_in_dim(padded, start_at.astype(jnp.int32), TIME_SAMPLES + TS, 1)
        blocks = shifted.reshape(2, N_TM + 1, TS)
        segments = jnp.concatenate([blocks[:, :-1], blocks[:, 1:]], axis=2)
        signal = lax.complex(segments[0], segments[1])
        response = lax.complex(jnp.cos(phase_row), jnp.sin(phase_row))
        spectrum = jnp.fft.fft(signal, axis=-1) * response[None, :]
        result = jnp.fft.ifft(spectrum, axis=-1)[:, TS:].reshape(TIME_SAMPLES)
        return jnp.stack([jnp.real(result), jnp.imag(result)])

    output_pair = lax.map(dedisperse_channel, (beam_sum, chirp_phase, offsets))
    output_pair = jnp.moveaxis(output_pair, 1, 0)
    dedispersed = output_pair.astype(jnp.bfloat16)
    power = output_pair[0] * output_pair[0] + output_pair[1] * output_pair[1]
    windows = power.reshape(CHANNEL_COUNT, NWIN, SKW)
    first_sum = jnp.sum(windows, axis=-1)
    second_sum = jnp.sum(windows * windows, axis=-1)
    kurtosis = (SKW + 1.0) / (SKW - 1.0) * (SKW * second_sum / (first_sum * first_sum + EPSILON) - 1.0)
    keep = (1 - flags).astype(jnp.float32)
    sk_weight = keep / (1.0 + ((kurtosis - 1.0) / SK_WIDTH) ** 2)
    weighted = (sk_weight[:, :, None] * windows).reshape(CHANNEL_COUNT, TIME_SAMPLES).astype(jnp.bfloat16)

    def fold_channel(row_values):
        return jax.ops.segment_sum(row_values.astype(jnp.float32), sample_phase_bins, BINS)

    profile = jax.vmap(fold_channel)(weighted) * (BINS / TIME_SAMPLES)
    band_profile = jnp.sum(profile, axis=0)
    return dedispersed, sk_weight, profile, band_profile
```

```python
import functools
import math

import jax
import jax.numpy as jnp
import numpy as np
from jax import lax
from jax.experimental import pallas as pl
from jax.experimental.pallas import tpu as pltpu
from jax.sharding import PartitionSpec as P

NFFT = 131072
OFFSET_BOUND = 4096
SKW = 1024
BINS = 2048


SK_WIDTH = 0.05
EPSILON = 1e-06

COLS = 1 << (NFFT.bit_length() - 1) // 2
ROWS = NFFT // COLS
HALF_ROWS = ROWS // 2
HALO_ROWS = OFFSET_BOUND // COLS
WIN_ROWS = SKW // COLS
WINDOWS = HALF_ROWS // WIN_ROWS
LOW_BINS = 32
HIGH_BINS = BINS // LOW_BINS
ROW_STEP = 8
LANES = 128
DEPTH = 256
PARTS = 4
PART_ROWS = HALF_ROWS // PARTS
MESH = pl.DeviceIdType.MESH


def bf16_split(table):
    high = table.astype(jnp.bfloat16)
    low = (table - high.astype(np.float32)).astype(jnp.bfloat16)
    return np.stack([high, low])


def dft_parts(length):
    index = np.arange(length, dtype=np.int64)
    angle = -2.0 * math.pi / length * (index[:, None] * index[None, :] % length)
    real, imag = (np.cos(angle).astype(np.float32), np.sin(angle).astype(np.float32))
    return np.stack([bf16_split(real), bf16_split(imag)])


def twiddle(row_total, col_total):
    turns = np.arange(row_total, dtype=np.int64)[:, None] * np.arange(col_total, dtype=np.int64) % NFFT
    angle = -2.0 * math.pi / NFFT * turns
    return np.stack([np.cos(angle), np.sin(angle)]).astype(np.float32)


def split(value):
    high = value.astype(jnp.bfloat16)
    return high, (value - high.astype(jnp.float32)).astype(jnp.bfloat16)


def three_pass(left, right, dims):
    def product(a, b):
        return lax.dot_general(a, b, (dims, ((), ())), preferred_element_type=jnp.float32)

    return product(left[0], right[0]) + (product(left[0], right[1]) + product(left[1], right[0]))


def table_times(table, pair, dims, sign):
    real, imag = (split(pair[0]), split(pair[1]))
    rr = three_pass(table[0], real, dims)
    ii = three_pass(table[1], imag, dims)
    ri = three_pass(table[0], imag, dims)
    ir = three_pass(table[1], real, dims)
    if sign > 0:
        return rr - ii, ri + ir
    return rr + ii, ri - ir


def cos_sin(angle):
    half = 0.5 * angle
    square = half * half
    sine = jnp.full_like(square, 1.0 / math.factorial(13))
    for power in (11, 9, 7, 5, 3, 1):
        sine = sine * square + (-1.0) ** (power // 2) / math.factorial(power)
    sine = sine * half
    cosine = jnp.full_like(square, 1.0 / math.factorial(12))
    for power in (10, 8, 6, 4, 2, 0):
        cosine = cosine * square + (-1.0) ** (power // 2) / math.factorial(power)
    return 1.0 - 2.0 * sine * sine, 2.0 * sine * cosine


def shifted_phase(phase, offset):
    high = lax.broadcasted_iota(jnp.int32, phase.shape, 0) * ROWS
    index = high + lax.broadcasted_iota(jnp.int32, phase.shape, 1)
    turns = (index * offset) & (NFFT - 1)
    turns = jnp.where(turns >= NFFT // 2, turns - NFFT, turns)
    phase = phase + turns.astype(jnp.float32) * (2.0 * math.pi / NFFT)
    phase = jnp.where(phase > math.pi, phase - 2.0 * math.pi, phase)
    return jnp.where(phase < -math.pi, phase + 2.0 * math.pi, phase)


def weight_table(gains_ref, table_ref, antennas, me):
    total = gains_ref.shape[2]
    lane = lax.broadcasted_iota(jnp.int32, (8, LANES), 1)
    wide = []
    for part in range(2):
        row = gains_ref[part]
        if total < LANES:
            row = jnp.concatenate([row, jnp.zeros((1, LANES - total), jnp.float32)], axis=1)
        row = jnp.broadcast_to(row, (8, LANES))
        row = pltpu.roll(row, lax.rem(LANES - me * antennas, LANES), 1)
        row = jnp.where(lane < antennas, row, 0.0)
        width = antennas
        while width < LANES:
            row = row + pltpu.roll(row, width, 1)
            width *= 2
        wide.append(jnp.concatenate([row] * (DEPTH // LANES), axis=1)[:1])
    real, imag = wide
    half = DEPTH // antennas // 2
    shape = (half, DEPTH)
    tile = lax.broadcasted_iota(jnp.int32, shape, 1) // antennas
    index = lax.broadcasted_iota(jnp.int32, shape, 0)
    for source, pair in enumerate(((real, imag), (-imag, real))):
        for out, values in enumerate(pair):
            for parity in range(2):
                dense = jnp.where(tile == 2 * index + parity, values, 0.0)
                high, low = split(dense)
                at = (2 * out + parity) * half
                table_ref[source, at : at + half] = high
                table_ref[source, 4 * half + at : 4 * half + at + half] = low


def part_beam(table_ref, volt_ref, antennas, put):
    half = DEPTH // antennas // 2
    groups = volt_ref.shape[1] // DEPTH
    joined = 2 if groups % 2 == 0 else 1
    for at in range(groups // joined):
        total = None
        for source in range(2):
            lanes = [
                volt_ref[source, (joined * at + b) * DEPTH : (joined * at + b + 1) * DEPTH]
                for b in range(joined)
            ]
            right = lanes[0] if joined == 1 else jnp.concatenate(lanes, axis=1)
            term = jnp.dot(table_ref[source], right, preferred_element_type=jnp.float32)
            total = term if total is None else total + term
        total = total[: 4 * half] + total[4 * half :]
        for b in range(joined):
            block = total[:, b * LANES : (b + 1) * LANES]
            for out in range(2):
                even = block[2 * out * half : (2 * out + 1) * half]
                odd = block[(2 * out + 1) * half : (2 * out + 2) * half]
                put(out, (joined * at + b) * half, half, jnp.concatenate([even, odd], axis=1))


def beam_kernel(
    antennas, pairs, volt_ref, gains_ref, wide_ref, table_ref, vbuf, pair_send, pair_recv,
    chip_send, chip_recv, own_ref, halo_ref, head_ref, load_sem, pair_sems, chip_sems, halo_sems,
    head_sems,
):
    count = 2 * pairs
    me = lax.axis_index("tm")
    pair, core = (me // 2, lax.rem(me, 2))
    barrier = pltpu.get_barrier_semaphore()
    for step in range(1, count):
        pl.semaphore_signal(
            barrier, inc=1, device_id={"tm": lax.rem(me + step, count)}, device_id_type=MESH
        )
    size = vbuf.shape[3]

    def shard_of(j, other):
        return lax.rem(pair + 1 + j, pairs) * 2 + (1 - core if other else core)

    def load(part, j, other):
        start = pl.multiple_of((shard_of(j, other) * PARTS + part) * size, size)
        slot = 2 * j + (0 if other else 1)
        return pltpu.make_async_copy(
            volt_ref.at[:, pl.ds(start, size)], vbuf.at[part, slot], load_sem.at[part, slot]
        )

    def order():
        return [(j, True) for j in range(pairs)] + [(j, False) for j in range(pairs)]

    def begin(part, carry):
        for j, other in order():
            load(part, j, other).start()
        return carry

    lax.fori_loop(0, PARTS, begin, 0)
    weight_table(gains_ref, table_ref, antennas, me)

    def pair_copy(part, j):
        return pltpu.make_async_remote_copy(
            src_ref=pair_send.at[part, j], dst_ref=pair_recv.at[part, j],
            send_sem=pair_sems.at[0, part, j], recv_sem=pair_sems.at[1, part, j],
            device_id={"tm": pair * 2 + (1 - core)}, device_id_type=MESH,
        )

    def chip_copy(part, j):
        return pltpu.make_async_remote_copy(
            src_ref=chip_send.at[part, j], dst_ref=chip_recv.at[part, j],
            send_sem=chip_sems.at[0, part, j], recv_sem=chip_sems.at[1, part, j],
            device_id={"tm": shard_of(j, False)}, device_id_type=MESH,
        )

    def halo_copy(part):
        return pltpu.make_async_remote_copy(
            src_ref=own_ref.at[part], dst_ref=halo_ref.at[part],
            send_sem=halo_sems.at[0, part], recv_sem=halo_sems.at[1, part],
            device_id={"tm": lax.rem(me + 1, count)}, device_id_type=MESH,
        )

    def head_copy():
        return pltpu.make_async_remote_copy(
            src_ref=own_ref.at[0, :, 0:HALO_ROWS], dst_ref=head_ref,
            send_sem=head_sems.at[0], recv_sem=head_sems.at[1],
            device_id={"tm": lax.rem(me + count - 1, count)}, device_id_type=MESH,
        )

    def finish(part):
        for j in range(pairs - 1):
            chip_copy(part, j).wait_recv()
        total = own_ref[part]
        for j in range(pairs - 1):
            total = total + chip_recv[part, j].astype(jnp.float32)
        own_ref[part] = total
        rows = pl.ds(pl.multiple_of(HALF_ROWS + part * PART_ROWS, PART_ROWS), PART_ROWS)
        wide_ref[:, rows] = total

        @pl.when(me < count - 1)
        def _():
            halo_copy(part).start()

    def run(part, carry):
        for j in range(pairs):
            load(part, j, True).wait()

            def put(out, at, rows, value, j=j):
                pair_send[part, j, out, at : at + rows] = value

            part_beam(table_ref, vbuf.at[part, 2 * j], antennas, put)
            if j == 0:

                @pl.when(part == 0)
                def _():
                    pl.semaphore_wait(barrier, count - 1)

            pair_copy(part, j).start()
        for j in range(pairs):
            load(part, j, False).wait()
            pair_copy(part, j).wait_recv()
            if j < pairs - 1:

                def put(out, at, rows, value, j=j):
                    value = value + pair_recv[part, j, out, at : at + rows]
                    chip_send[part, j, out, at : at + rows] = value.astype(jnp.bfloat16)

            else:

                def put(out, at, rows, value, j=j):
                    value = value + pair_recv[part, j, out, at : at + rows]
                    own_ref[part, out, at : at + rows] = value

            part_beam(table_ref, vbuf.at[part, 2 * j + 1], antennas, put)
            if j < pairs - 1:
                chip_copy(part, j).start()

        @pl.when(part > 0)
        def _():
            finish(part - 1)

            @pl.when((part == 1) & (me > 0))
            def _():
                head_copy().start()

        return carry

    lax.fori_loop(0, PARTS, run, 0)
    finish(PARTS - 1)

    @pl.when(me > 0)
    def _():
        for part in range(PARTS):
            halo_copy(part).wait_recv()
            wide_ref[:, part * PART_ROWS : (part + 1) * PART_ROWS] = halo_ref[part]
        head_copy().wait_send()

    @pl.when(me == 0)
    def _():
        wide_ref[:, 0:HALF_ROWS] = jnp.zeros((2, HALF_ROWS, COLS), jnp.float32)

    @pl.when(me < count - 1)
    def _():
        head_copy().wait_recv()
        wide_ref[:, ROWS : ROWS + HALO_ROWS] = head_ref[...]
        for part in range(PARTS):
            halo_copy(part).wait_send()

    @pl.when(me == count - 1)
    def _():
        wide_ref[:, ROWS : ROWS + HALO_ROWS] = jnp.zeros((2, HALO_ROWS, COLS), jnp.float32)

    def drain(part, carry):
        for j in range(pairs):
            pair_copy(part, j).wait_send()
            if j < pairs - 1:
                chip_copy(part, j).wait_send()
        return carry

    lax.fori_loop(0, PARTS, drain, 0)


def beam(volts, gains, antennas, shards):
    pairs = shards // 2
    size = volts.shape[1] // shards // PARTS
    half = DEPTH // antennas // 2
    block = (2, PART_ROWS, COLS)
    vmem = pl.BlockSpec(memory_space=pltpu.VMEM)
    return pl.pallas_call(
        functools.partial(beam_kernel, antennas, pairs),
        out_shape=jax.ShapeDtypeStruct((2, ROWS + HALO_ROWS, COLS), jnp.float32),
        in_specs=[pl.BlockSpec(memory_space=pl.ANY), vmem],
        out_specs=vmem,
        scratch_shapes=[
            pltpu.VMEM((2, 8 * half, DEPTH), jnp.bfloat16),
            pltpu.VMEM((PARTS, shards, 2, size, LANES), jnp.bfloat16),
            pltpu.VMEM((PARTS, pairs) + block, jnp.float32),
            pltpu.VMEM((PARTS, pairs) + block, jnp.float32),
            pltpu.VMEM((PARTS, pairs - 1) + block, jnp.bfloat16),
            pltpu.VMEM((PARTS, pairs - 1) + block, jnp.bfloat16),
            pltpu.VMEM((PARTS,) + block, jnp.float32),
            pltpu.VMEM((PARTS,) + block, jnp.float32),
            pltpu.VMEM((2, HALO_ROWS, COLS), jnp.float32),
            pltpu.SemaphoreType.DMA((PARTS, shards)),
            pltpu.SemaphoreType.DMA((2, PARTS, pairs)),
            pltpu.SemaphoreType.DMA((2, PARTS, pairs - 1)),
            pltpu.SemaphoreType.DMA((2, PARTS)),
            pltpu.SemaphoreType.DMA((2,)),
        ],
        compiler_params=pltpu.CompilerParams(
            vmem_limit_bytes=40 << 20, collective_id=0, has_side_effects=True
        ),
        cost_estimate=pl.CostEstimate(
            flops=3 * 10**9, bytes_accessed=18 << 20, transcendentals=0
        ),
        name="beam",
    )(volts, gains)


def fold_kernel(
    chans, shards, offset_ref, wide_ref, chirp_ref, keep_ref, bins_ref, outer_ref, inner_ref,
    twist_ref, twist_back_ref, dedispersed_ref, weight_ref, profile_ref, band_ref, weighted_ref,
    send_ref, recv_ref, sems,
):
    everyone = chans * shards
    here = lax.axis_index("chan") * shards + lax.axis_index("tm")
    barrier = pltpu.get_barrier_semaphore()

    def target(index):
        return {"chan": index // shards, "tm": lax.rem(index, shards)}

    def greet(step, carry):
        pl.semaphore_signal(
            barrier, inc=1, device_id=target(lax.rem(here + step, everyone)), device_id_type=MESH
        )
        return carry

    lax.fori_loop(1, everyone, greet, 0)
    offset = offset_ref[0]
    spot = lax.broadcasted_iota(jnp.int32, (HALO_ROWS, COLS), 0) * COLS
    spot = spot + lax.broadcasted_iota(jnp.int32, (HALO_ROWS, COLS), 1)
    signal = []
    for half in range(2):
        first = jnp.where(spot < offset, wide_ref[half, ROWS:], wide_ref[half, :HALO_ROWS])
        signal.append(jnp.concatenate([first, wide_ref[half, HALO_ROWS:ROWS]], axis=0))

    def table(ref, rows=slice(None)):
        return [[ref[0, 0, rows], ref[0, 1, rows]], [ref[1, 0, rows], ref[1, 1, rows]]]

    plain, turned = (((1,), (0,)), ((1,), (1,)))
    real, imag = table_times(table(outer_ref), signal, plain, 1)
    cosine, sine = (twist_ref[0], twist_ref[1])
    real, imag = (real * cosine - imag * sine, real * sine + imag * cosine)
    real, imag = table_times(table(inner_ref), (real, imag), turned, 1)
    cosine, sine = cos_sin(shifted_phase(chirp_ref[...], offset))
    real, imag = (real * cosine - imag * sine, real * sine + imag * cosine)
    real, imag = table_times(table(inner_ref), (real, imag), plain, -1)
    cosine, sine = (twist_back_ref[0], twist_back_ref[1])
    real, imag = (real * cosine + imag * sine, imag * cosine - real * sine)
    real, imag = table_times(
        table(outer_ref, slice(HALF_ROWS, ROWS)), (real, imag), turned, -1
    )
    real, imag = (real * (1.0 / NFFT), imag * (1.0 / NFFT))
    dedispersed_ref[0] = real.astype(jnp.bfloat16)
    dedispersed_ref[1] = imag.astype(jnp.bfloat16)
    power = real * real + imag * imag

    def exact_dot(a, b):
        return jnp.dot(a, b, precision=lax.Precision.HIGHEST, preferred_element_type=jnp.float32)

    def owner(shape, axis):
        rows = lax.broadcasted_iota(jnp.int32, shape, axis)
        windows = lax.broadcasted_iota(jnp.int32, shape, 1 - axis)
        return jnp.where(rows // WIN_ROWS == windows, 1.0, 0.0).astype(jnp.float32)

    gather = owner((WINDOWS, HALF_ROWS), 1)
    first_sum = jnp.sum(exact_dot(gather, power), axis=1, keepdims=True)
    second_sum = jnp.sum(exact_dot(gather, power * power), axis=1, keepdims=True)
    kurtosis = (
        (SKW + 1.0) / (SKW - 1.0) * (SKW * second_sum / (first_sum * first_sum + EPSILON) - 1.0)
    )
    scaled = (kurtosis - 1.0) / SK_WIDTH
    sk_weight = keep_ref[...] / (1.0 + scaled * scaled)
    sk_weight = jnp.broadcast_to(sk_weight, (WINDOWS, COLS))
    weight_ref[...] = sk_weight[:, :128]
    spread_weight = exact_dot(owner((HALF_ROWS, WINDOWS), 0), sk_weight)
    weighted_ref[...] = (spread_weight * power).astype(jnp.bfloat16).astype(jnp.float32)

    high_index = lax.broadcasted_iota(jnp.int32, (HIGH_BINS, LANES), 0)
    low_index = lax.broadcasted_iota(jnp.int32, (LOW_BINS, LANES), 0)

    def step(at, total):
        rows = pl.ds(pl.multiple_of(at * ROW_STEP, ROW_STEP), ROW_STEP)
        wide_rows = pl.ds(pl.multiple_of(at * 2 * ROW_STEP, 2 * ROW_STEP), 2 * ROW_STEP)
        bins, values = (bins_ref[wide_rows, :], weighted_ref[rows, :])
        high, low = (bins // LOW_BINS, bins % LOW_BINS)
        left, right = ([], [])
        for row in range(2 * ROW_STEP):
            value = values[row // 2 : row // 2 + 1, row % 2 * LANES : (row % 2 + 1) * LANES]
            left.append(
                jnp.where(high_index == high[row : row + 1], 1.0, 0.0).astype(jnp.bfloat16)
            )
            right.append(
                jnp.where(low_index == low[row : row + 1], value, 0.0).astype(jnp.bfloat16)
            )
        return total + lax.dot_general(
            jnp.concatenate(left, axis=1),
            jnp.concatenate(right, axis=1),
            (turned, ((), ())),
            preferred_element_type=jnp.float32,
        )

    total = lax.fori_loop(
        0, HALF_ROWS // ROW_STEP, step, jnp.zeros((HIGH_BINS, LOW_BINS), jnp.float32)
    )
    per_row = LANES // LOW_BINS
    total = jnp.concatenate([total, jnp.zeros((HIGH_BINS, LANES - LOW_BINS), jnp.float32)], axis=1)
    place = lax.broadcasted_iota(jnp.int32, (HIGH_BINS, LANES), 0) % per_row
    moved = jnp.where(place == 0, total, 0.0)
    for at in range(1, per_row):
        moved = moved + jnp.where(place == at, pltpu.roll(total, at * LOW_BINS, 1), 0.0)
    lines = BINS // LANES // shards
    for line in range(BINS // LANES):
        send_ref[line // lines, line % lines : line % lines + 1] = jnp.sum(
            moved[line * per_row : (line + 1) * per_row], axis=0, keepdims=True
        )
    pl.semaphore_wait(barrier, everyone - 1)

    def outgoing(index):
        return pltpu.make_async_remote_copy(
            src_ref=send_ref.at[lax.rem(index, shards)], dst_ref=recv_ref.at[here],
            send_sem=sems.at[0, index], recv_sem=sems.at[1, here],
            device_id=target(index), device_id_type=MESH,
        )

    def incoming(index):
        return pltpu.make_async_remote_copy(
            src_ref=send_ref.at[lax.rem(index, shards)], dst_ref=recv_ref.at[index],
            send_sem=sems.at[0, index], recv_sem=sems.at[1, index],
            device_id=target(index), device_id_type=MESH,
        )

    def begin(step, carry):
        outgoing(lax.rem(here + step, everyone)).start()
        return carry

    def arrive(step, carry):
        incoming(lax.rem(here + everyone - step, everyone)).wait_recv()
        return carry

    def leave(step, carry):
        outgoing(lax.rem(here + step, everyone)).wait_send()
        return carry

    lax.fori_loop(1, everyone, begin, 0)
    recv_ref[here] = send_ref[lax.axis_index("tm")]
    lax.fori_loop(1, everyone, arrive, 0)
    scale = BINS / (HALF_ROWS * COLS * shards)
    band = None
    mine = lax.axis_index("chan")
    for chan in range(chans):
        line = recv_ref[chan * shards]
        for at in range(1, shards):
            line = line + recv_ref[chan * shards + at]
        line = line * scale
        own = jnp.where(mine == chan, line, 0.0)
        band, profile = (line, own) if band is None else (band + line, profile + own)
    profile_ref[...] = profile
    band_ref[...] = band
    lax.fori_loop(1, everyone, leave, 0)


def fold(offset, wide, chirp, keep, bins, chans, shards):
    vmem = pl.BlockSpec(memory_space=pltpu.VMEM)
    tables = (dft_parts(ROWS), dft_parts(COLS), twiddle(ROWS, COLS), twiddle(COLS, ROWS))
    lines = BINS // LANES // shards
    line = jax.ShapeDtypeStruct((lines, LANES), jnp.float32)
    return pl.pallas_call(
        functools.partial(fold_kernel, chans, shards),
        out_shape=(
            jax.ShapeDtypeStruct((2, HALF_ROWS, COLS), jnp.bfloat16),
            jax.ShapeDtypeStruct((WINDOWS, 128), jnp.float32),
            line,
            line,
        ),
        in_specs=[pl.BlockSpec(memory_space=pltpu.SMEM)] + [vmem] * 8,
        out_specs=(vmem,) * 4,
        scratch_shapes=[
            pltpu.VMEM((HALF_ROWS, COLS), jnp.float32),
            pltpu.VMEM((shards, lines, LANES), jnp.float32),
            pltpu.VMEM((chans * shards, lines, LANES), jnp.float32),
            pltpu.SemaphoreType.DMA((2, chans * shards)),
        ],
        compiler_params=pltpu.CompilerParams(
            vmem_limit_bytes=40 << 20, collective_id=1, has_side_effects=True
        ),
        cost_estimate=pl.CostEstimate(
            flops=6 * 10**9, bytes_accessed=6 << 20, transcendentals=0
        ),
        name="fold",
    )(offset, wide, chirp, keep, bins, *[jnp.asarray(table) for table in tables])


def on_device(voltages, antenna_gains, chirp_phase, offsets, flags, sample_phase_bins):
    shards, chans = (lax.axis_size("tm"), lax.axis_size("chan"))
    antennas, channels, samples = voltages.shape[1:]
    assert channels == 1 and shards % 2 == 0
    volts = voltages.reshape(2, antennas, samples // LANES, LANES)
    volts = jnp.transpose(volts, (0, 2, 1, 3)).reshape(2, samples // LANES * antennas, LANES)
    gains = jnp.transpose(antenna_gains, (0, 2, 1))
    wide = beam(volts, gains, antennas, shards)
    chirp = chirp_phase.reshape(COLS, ROWS)
    keep = (1 - flags).astype(jnp.float32).reshape(WINDOWS, 1)
    bins = sample_phase_bins.reshape(-1, LANES)
    dedispersed, weight, profile, band = fold(offsets, wide, chirp, keep, bins, chans, shards)
    return (
        dedispersed.reshape(2, 1, HALF_ROWS * COLS),
        weight[:, 0].reshape(1, WINDOWS),
        profile.reshape(1, BINS // shards),
        band.reshape(BINS // shards),
    )


def solution(mesh):
    placed = (
        P(None, "tm", "chan", None),
        P(None, None, "chan"),
        P("chan", None),
        P("chan"),
        P("chan", "tm"),
        P("tm"),
    )
    return jax.shard_map(
        on_device,
        mesh=mesh,
        in_specs=placed,
        out_specs=(P(None, "chan", "tm"), P("chan", "tm"), P("chan", "tm"), P("tm")),
        check_vma=False,
    )
```

```python
import functools
import math

import jax
import jax.numpy as jnp
import numpy as np
from jax import lax
from jax.experimental import pallas as pl
from jax.experimental.pallas import tpu as pltpu
from jax.sharding import PartitionSpec as P

NFFT = 131072
OFFSET_BOUND = 4096
SKW = 1024
BINS = 2048


SK_WIDTH = 0.05
EPSILON = 1e-06

COLS = 1 << (NFFT.bit_length() - 1) // 2
ROWS = NFFT // COLS
HALF_ROWS = ROWS // 2
HALO_ROWS = OFFSET_BOUND // COLS
WIN_ROWS = SKW // COLS
WINDOWS = HALF_ROWS // WIN_ROWS
LOW_BINS = 32
HIGH_BINS = BINS // LOW_BINS
BLOCK_ROWS = 128
STEP_LINES = 32
LANES = 128
DEPTH = 256
PARTS = 4
PART_ROWS = HALF_ROWS // PARTS
MESH = pl.DeviceIdType.MESH


def bf16_split(table):
    high = table.astype(jnp.bfloat16)
    low = (table - high.astype(np.float32)).astype(jnp.bfloat16)
    return np.stack([high, low])


def unit_roots(turns, period):
    angle = -2.0 * math.pi / period * (turns % period)
    return (np.cos(angle).astype(np.float32), np.sin(angle).astype(np.float32))


def dft_table():
    index = np.arange(COLS, dtype=np.int64)
    real, imag = unit_roots(index[:, None] * index[None, :], COLS)
    return np.stack([bf16_split(real), bf16_split(imag), bf16_split(-imag)])


def twiddle():
    index = np.arange(HALF_ROWS, dtype=np.int64)
    rows = np.stack([2 * index, 2 * index + 1])
    return np.stack(unit_roots(rows[:, :, None] * np.arange(COLS, dtype=np.int64), NFFT))


def half_turns():
    index = np.arange(HALF_ROWS, dtype=np.int64)
    return np.stack(unit_roots(np.repeat(index[:, None], LANES, axis=1), ROWS))


def split(value):
    high = value.astype(jnp.bfloat16)
    return high, (value - high.astype(jnp.float32)).astype(jnp.bfloat16)


def product(*pairs):
    left, right = ([], [])
    for a, b in pairs:
        left += [a[0], a[0], a[1]]
        right += [b[0], b[1], b[0]]
    return jnp.dot(
        jnp.concatenate(left, axis=1),
        jnp.concatenate(right, axis=0),
        preferred_element_type=jnp.float32,
    )


def cos_sin(angle):
    half = 0.5 * angle
    square = half * half
    sine = jnp.full_like(square, 1.0 / math.factorial(13))
    for power in (11, 9, 7, 5, 3, 1):
        sine = sine * square + (-1.0) ** (power // 2) / math.factorial(power)
    sine = sine * half
    cosine = jnp.full_like(square, 1.0 / math.factorial(12))
    for power in (10, 8, 6, 4, 2, 0):
        cosine = cosine * square + (-1.0) ** (power // 2) / math.factorial(power)
    return 1.0 - 2.0 * sine * sine, 2.0 * sine * cosine


def response(phase, first, first_column, offset):
    index = first + lax.broadcasted_iota(jnp.int32, phase.shape, 0)
    column = first_column + lax.broadcasted_iota(jnp.int32, phase.shape, 1)
    index = index + ROWS * column
    turns = (index * offset) & (NFFT - 1)
    turns = jnp.where(turns >= NFFT // 2, turns - NFFT, turns)
    phase = phase + turns.astype(jnp.float32) * (2.0 * math.pi / NFFT)
    phase = jnp.where(phase > math.pi, phase - 2.0 * math.pi, phase)
    phase = jnp.where(phase < -math.pi, phase + 2.0 * math.pi, phase)
    return cos_sin(phase)


def weight_table(gains_ref, table_ref, antennas, me):
    total = gains_ref.shape[2]
    lane = lax.broadcasted_iota(jnp.int32, (8, LANES), 1)
    wide = []
    for part in range(2):
        row = gains_ref[part]
        if total < LANES:
            row = jnp.concatenate([row, jnp.zeros((1, LANES - total), jnp.float32)], axis=1)
        row = jnp.broadcast_to(row, (8, LANES))
        row = pltpu.roll(row, lax.rem(LANES - me * antennas, LANES), 1)
        row = jnp.where(lane < antennas, row, 0.0)
        width = antennas
        while width < LANES:
            row = row + pltpu.roll(row, width, 1)
            width *= 2
        wide.append(jnp.concatenate([row] * (DEPTH // LANES), axis=1)[:1])
    real, imag = wide
    half = DEPTH // antennas // 2
    shape = (half, DEPTH)
    tile = lax.broadcasted_iota(jnp.int32, shape, 1) // antennas
    index = lax.broadcasted_iota(jnp.int32, shape, 0)
    for source, pair in enumerate(((real, imag), (-imag, real))):
        for out, values in enumerate(pair):
            for parity in range(2):
                dense = jnp.where(tile == 2 * index + parity, values, 0.0)
                high, low = split(dense)
                at = (2 * out + parity) * half
                table_ref[source, at : at + half] = high
                table_ref[source, 4 * half + at : 4 * half + at + half] = low


def part_beam(table_ref, volt_ref, antennas, put):
    half = DEPTH // antennas // 2
    groups = volt_ref.shape[1] // DEPTH
    joined = 2 if groups % 2 == 0 else 1
    for at in range(groups // joined):
        total = None
        for source in range(2):
            lanes = [
                volt_ref[source, (joined * at + b) * DEPTH : (joined * at + b + 1) * DEPTH]
                for b in range(joined)
            ]
            right = lanes[0] if joined == 1 else jnp.concatenate(lanes, axis=1)
            term = jnp.dot(table_ref[source], right, preferred_element_type=jnp.float32)
            total = term if total is None else total + term
        total = total[: 4 * half] + total[4 * half :]
        for b in range(joined):
            block = total[:, b * LANES : (b + 1) * LANES]
            for out in range(2):
                even = block[2 * out * half : (2 * out + 1) * half]
                odd = block[(2 * out + 1) * half : (2 * out + 2) * half]
                put(out, (joined * at + b) * half, half, jnp.concatenate([even, odd], axis=1))


def beam_kernel(
    antennas, pairs, volt_ref, gains_ref, offset_ref, chirp_hbm, turns_hbm, data_ref, response_ref,
    table_ref, vbuf, pair_send, pair_recv, chip_send, chip_recv, own_ref, halo_send, halo_ref,
    head_ref, chirp_ref, turns_ref, block_ref, load_sem, pair_sems, chip_sems, halo_sems,
    head_sems, side_sems,
):
    count = 2 * pairs
    me = lax.axis_index("tm")
    pair, core = (me // 2, lax.rem(me, 2))
    barrier = pltpu.get_barrier_semaphore()
    for step in range(1, count):
        pl.semaphore_signal(
            barrier, inc=1, device_id={"tm": lax.rem(me + step, count)}, device_id_type=MESH
        )
    size = vbuf.shape[3]

    def shard_of(j, other):
        return lax.rem(pair + 1 + j, pairs) * 2 + (1 - core if other else core)

    def load(part, j, other):
        start = pl.multiple_of((shard_of(j, other) * PARTS + part) * size, size)
        slot = 2 * j + (0 if other else 1)
        return pltpu.make_async_copy(
            volt_ref.at[:, pl.ds(start, size)], vbuf.at[part, slot], load_sem.at[part, slot]
        )

    def order():
        return [(j, True) for j in range(pairs)] + [(j, False) for j in range(pairs)]

    def begin(part, carry):
        for j, other in order():
            load(part, j, other).start()
        return carry

    lax.fori_loop(0, PARTS, begin, 0)
    side = [
        pltpu.make_async_copy(chirp_hbm, chirp_ref, side_sems.at[0]),
        pltpu.make_async_copy(turns_hbm, turns_ref, side_sems.at[1]),
    ]
    for copy in side:
        copy.start()
    offset = offset_ref[0]
    weight_table(gains_ref, table_ref, antennas, me)

    def pair_copy(part, j):
        return pltpu.make_async_remote_copy(
            src_ref=pair_send.at[part, j], dst_ref=pair_recv.at[part, j],
            send_sem=pair_sems.at[0, part, j], recv_sem=pair_sems.at[1, part, j],
            device_id={"tm": pair * 2 + (1 - core)}, device_id_type=MESH,
        )

    def chip_copy(part, j):
        return pltpu.make_async_remote_copy(
            src_ref=chip_send.at[part, j], dst_ref=chip_recv.at[part, j],
            send_sem=chip_sems.at[0, part, j], recv_sem=chip_sems.at[1, part, j],
            device_id={"tm": shard_of(j, False)}, device_id_type=MESH,
        )

    def halo_copy(part):
        return pltpu.make_async_remote_copy(
            src_ref=halo_send.at[part], dst_ref=halo_ref.at[part],
            send_sem=halo_sems.at[0, part], recv_sem=halo_sems.at[1, part],
            device_id={"tm": lax.rem(me + 1, count)}, device_id_type=MESH,
        )

    def head_copy():
        return pltpu.make_async_remote_copy(
            src_ref=halo_send.at[0, :, 0:HALO_ROWS], dst_ref=head_ref,
            send_sem=head_sems.at[0], recv_sem=head_sems.at[1],
            device_id={"tm": lax.rem(me + count - 1, count)}, device_id_type=MESH,
        )

    def finish(part):
        for j in range(pairs - 1):
            chip_copy(part, j).wait_recv()
        total = own_ref[part]
        for j in range(pairs - 1):
            total = total + chip_recv[part, j].astype(jnp.float32)
        own_ref[part] = total
        halo_send[part] = total.astype(jnp.bfloat16)

        @pl.when(me < count - 1)
        def _():
            halo_copy(part).start()

    def chirp_block(at):
        stride = ROWS // LANES
        for half in range(COLS // LANES):
            columns = chirp_ref[
                pl.ds(at + half * LANES * stride, LANES, stride=stride), :
            ]
            phase = jnp.transpose(columns, (1, 0))
            for out, value in enumerate(response(phase, at * LANES, half * LANES, offset)):
                block_ref[...] = value * (1.0 / NFFT)
                for parity in range(2):
                    rows = pl.ds(pl.multiple_of(at * (LANES // 2), LANES // 2), LANES // 2)
                    response_ref[out, parity, rows, half * LANES : (half + 1) * LANES] = (
                        block_ref[pl.ds(parity, LANES // 2, stride=2), :]
                    )

    def combine(part, first=None):
        rows = slice(part * PART_ROWS, (part + 1) * PART_ROWS)
        before = [halo_ref[part, out].astype(jnp.float32) for out in range(2)]
        if first is not None:
            before = [
                jnp.concatenate([head, value[HALO_ROWS:]], axis=0)
                for head, value in zip(first, before)
            ]
        after = [own_ref[part, 0], own_ref[part, 1]]
        real, imag = (before[0] - after[0], before[1] - after[1])
        cosine, sine = [
            jnp.concatenate([turns_ref[out, rows]] * (COLS // LANES), axis=1) for out in range(2)
        ]
        both = (
            (before[0] + after[0], before[1] + after[1]),
            (real * cosine - imag * sine, real * sine + imag * cosine),
        )
        for kind, values in enumerate(both):
            for out, value in enumerate(values):
                data_ref[kind, out, 0, rows], data_ref[kind, out, 1, rows] = split(value)

    def run(part, carry):
        for j in range(pairs):
            load(part, j, True).wait()

            def put(out, at, rows, value, j=j):
                pair_send[part, j, out, at : at + rows] = value

            part_beam(table_ref, vbuf.at[part, 2 * j], antennas, put)
            if j == 0:

                @pl.when(part == 0)
                def _():
                    pl.semaphore_wait(barrier, count - 1)

            pair_copy(part, j).start()
        for j in range(pairs):
            load(part, j, False).wait()
            pair_copy(part, j).wait_recv()
            if j < pairs - 1:

                def put(out, at, rows, value, j=j):
                    value = value + pair_recv[part, j, out, at : at + rows]
                    chip_send[part, j, out, at : at + rows] = value.astype(jnp.bfloat16)

            else:

                def put(out, at, rows, value, j=j):
                    value = value + pair_recv[part, j, out, at : at + rows]
                    own_ref[part, out, at : at + rows] = value

            part_beam(table_ref, vbuf.at[part, 2 * j + 1], antennas, put)
            if j < pairs - 1:
                chip_copy(part, j).start()

        @pl.when(part == 0)
        def _():
            for copy in side:
                copy.wait()

        chirp_block(part)

        @pl.when(part > 0)
        def _():
            finish(part - 1)

            @pl.when((part == 1) & (me > 0))
            def _():
                head_copy().start()

        return carry

    lax.fori_loop(0, PARTS, run, 0)
    finish(PARTS - 1)

    @pl.when(me == 0)
    def _():
        halo_ref[...] = jnp.zeros((PARTS, 2, PART_ROWS, COLS), jnp.bfloat16)

    @pl.when(me == count - 1)
    def _():
        head_ref[...] = jnp.zeros((2, HALO_ROWS, COLS), jnp.bfloat16)

    for part in range(PARTS):

        @pl.when(me > 0)
        def _():
            halo_copy(part).wait_recv()

        first = None
        if part == 0:

            @pl.when(me < count - 1)
            def _():
                head_copy().wait_recv()

            spot = lax.broadcasted_iota(jnp.int32, (HALO_ROWS, COLS), 0) * COLS
            spot = spot + lax.broadcasted_iota(jnp.int32, (HALO_ROWS, COLS), 1)
            first = [
                jnp.where(
                    spot < offset,
                    head_ref[out].astype(jnp.float32),
                    halo_ref[0, out, 0:HALO_ROWS].astype(jnp.float32),
                )
                for out in range(2)
            ]
        combine(part, first)

    @pl.when(me > 0)
    def _():
        head_copy().wait_send()

    @pl.when(me < count - 1)
    def _():
        for part in range(PARTS):
            halo_copy(part).wait_send()

    def drain(part, carry):
        for j in range(pairs):
            pair_copy(part, j).wait_send()
            if j < pairs - 1:
                chip_copy(part, j).wait_send()
        return carry

    lax.fori_loop(0, PARTS, drain, 0)


def beam(volts, gains, offset, chirp, shards):
    pairs = shards // 2
    size = volts.shape[1] // shards // PARTS
    antennas = size * LANES // (PART_ROWS * COLS)
    half = DEPTH // antennas // 2
    block = (2, PART_ROWS, COLS)
    vmem = pl.BlockSpec(memory_space=pltpu.VMEM)
    hbm = pl.BlockSpec(memory_space=pl.ANY)
    return pl.pallas_call(
        functools.partial(beam_kernel, antennas, pairs),
        out_shape=(
            jax.ShapeDtypeStruct((2, 2, 2, HALF_ROWS, COLS), jnp.bfloat16),
            jax.ShapeDtypeStruct((2, 2, HALF_ROWS, COLS), jnp.float32),
        ),
        in_specs=[hbm, vmem, pl.BlockSpec(memory_space=pltpu.SMEM), hbm, hbm],
        out_specs=(vmem, vmem),
        scratch_shapes=[
            pltpu.VMEM((2, 8 * half, DEPTH), jnp.bfloat16),
            pltpu.VMEM((PARTS, shards, 2, size, LANES), jnp.bfloat16),
            pltpu.VMEM((PARTS, pairs) + block, jnp.float32),
            pltpu.VMEM((PARTS, pairs) + block, jnp.float32),
            pltpu.VMEM((PARTS, pairs - 1) + block, jnp.bfloat16),
            pltpu.VMEM((PARTS, pairs - 1) + block, jnp.bfloat16),
            pltpu.VMEM((PARTS,) + block, jnp.float32),
            pltpu.VMEM((PARTS,) + block, jnp.bfloat16),
            pltpu.VMEM((PARTS,) + block, jnp.bfloat16),
            pltpu.VMEM((2, HALO_ROWS, COLS), jnp.bfloat16),
            pltpu.VMEM((NFFT // LANES, LANES), jnp.float32),
            pltpu.VMEM((2, HALF_ROWS, LANES), jnp.float32),
            pltpu.VMEM((LANES, LANES), jnp.float32),
            pltpu.SemaphoreType.DMA((PARTS, shards)),
            pltpu.SemaphoreType.DMA((2, PARTS, pairs)),
            pltpu.SemaphoreType.DMA((2, PARTS, pairs - 1)),
            pltpu.SemaphoreType.DMA((2, PARTS)),
            pltpu.SemaphoreType.DMA((2,)),
            pltpu.SemaphoreType.DMA((2,)),
        ],
        compiler_params=pltpu.CompilerParams(
            vmem_limit_bytes=44 << 20, collective_id=0, has_side_effects=True
        ),
        cost_estimate=pl.CostEstimate(
            flops=3 * 10**9, bytes_accessed=18 << 20, transcendentals=0
        ),
        name="beam",
    )(volts, gains, offset, chirp, jnp.asarray(half_turns()))


def fold_kernel(
    chans, shards, data_ref, response_ref, flags_ref, bins_ref, dft_ref, twist_ref, turns_ref,
    dedispersed_ref, small_ref, back_ref, weighted_ref, high_ref, low_ref, send_ref, recv_ref,
    sems,
):
    everyone = chans * shards
    here = lax.axis_index("chan") * shards + lax.axis_index("tm")
    barrier = pltpu.get_barrier_semaphore()

    def target(index):
        return {"chan": index // shards, "tm": lax.rem(index, shards)}

    def greet(step, carry):
        pl.semaphore_signal(
            barrier, inc=1, device_id=target(lax.rem(here + step, everyone)), device_id_type=MESH
        )
        return carry

    lax.fori_loop(1, everyone, greet, 0)
    def table(at):
        return (dft_ref[at, 0], dft_ref[at, 1])

    real_table, imag_table, minus_table = (table(0), table(1), table(2))

    def ahead(tables, at):
        return tuple(half[at] for half in tables)

    for kind in range(2):
        given = [(data_ref[kind, out, 0], data_ref[kind, out, 1]) for out in range(2)]
        for start in range(0, HALF_ROWS, BLOCK_ROWS):
            rows = slice(start, start + BLOCK_ROWS)
            left, cross, minus = (
                ahead(real_table, rows), ahead(imag_table, rows), ahead(minus_table, rows)
            )
            real = product((left, given[0]), (minus, given[1]))
            imag = product((left, given[1]), (cross, given[0]))
            cosine, sine = (twist_ref[0, kind, rows], twist_ref[1, kind, rows])
            pair = (split(real * cosine - imag * sine), split(real * sine + imag * cosine))
            real = product((pair[0], real_table), (pair[1], minus_table))
            imag = product((pair[0], imag_table), (pair[1], real_table))
            turn, tilt = (response_ref[0, kind, rows], response_ref[1, kind, rows])
            pair = (split(real * turn - imag * tilt), split(real * tilt + imag * turn))
            real = product((pair[0], real_table), (pair[1], imag_table))
            imag = product((pair[0], minus_table), (pair[1], real_table))
            for out, value in enumerate(
                (real * cosine + imag * sine, imag * cosine - real * sine)
            ):
                back_ref[kind, out, 0, rows], back_ref[kind, out, 1, rows] = split(value)

    flag = flags_ref[...]
    if WINDOWS < LANES:
        flag = jnp.concatenate([flag, jnp.zeros((1, LANES - WINDOWS), jnp.int32)], axis=1)
    keep_row = (1 - flag).astype(jnp.float32)
    shape = (BLOCK_ROWS, LANES)
    row_index = lax.broadcasted_iota(jnp.int32, shape, 0)
    lane_index = lax.broadcasted_iota(jnp.int32, shape, 1)

    def window_sum(values):
        total = jnp.broadcast_to(jnp.sum(values, axis=1, keepdims=True), shape)
        reach = 1
        while reach < WIN_ROWS:
            up, down = (pltpu.roll(total, BLOCK_ROWS - reach, 0), pltpu.roll(total, reach, 0))
            total = total + jnp.where(row_index % (2 * reach) < reach, up, down)
            reach *= 2
        return total

    per_line = COLS // LANES
    weight_row = jnp.zeros((1, LANES), jnp.float32)
    for start in range(0, HALF_ROWS, BLOCK_ROWS):
        rows = slice(start, start + BLOCK_ROWS)
        left, cross, minus = (
            ahead(real_table, rows), ahead(imag_table, rows), ahead(minus_table, rows)
        )
        parts = []
        for kind in range(2):
            given = [(back_ref[kind, out, 0], back_ref[kind, out, 1]) for out in range(2)]
            parts.append(
                (
                    product((left, given[0]), (cross, given[1])),
                    product((left, given[1]), (minus, given[0])),
                )
            )
        cosine, sine = [
            jnp.concatenate([turns_ref[out, rows]] * (COLS // LANES), axis=1) for out in range(2)
        ]
        (real, imag), (odd_real, odd_imag) = parts
        real = real - (odd_real * cosine + odd_imag * sine)
        imag = imag - (odd_imag * cosine - odd_real * sine)
        dedispersed_ref[0, rows] = real.astype(jnp.bfloat16)
        dedispersed_ref[1, rows] = imag.astype(jnp.bfloat16)
        power = real * real + imag * imag
        first_sum, second_sum = (window_sum(power), window_sum(power * power))
        kurtosis = (
            (SKW + 1.0)
            / (SKW - 1.0)
            * (SKW * second_sum / (first_sum * first_sum + EPSILON) - 1.0)
        )
        scaled = (kurtosis - 1.0) / SK_WIDTH
        window = (row_index + start) // WIN_ROWS
        keep = jnp.where(lane_index == window, jnp.broadcast_to(keep_row, shape), 0.0)
        keep = jnp.sum(keep, axis=1, keepdims=True)
        sk_weight = keep / (1.0 + scaled * scaled)
        chosen = (row_index + start) == lane_index * WIN_ROWS
        weight_row = weight_row + jnp.sum(
            jnp.where(chosen, sk_weight, 0.0), axis=0, keepdims=True
        )
        for at in range(COLS // LANES):
            lanes = slice(at * LANES, (at + 1) * LANES)
            value = (sk_weight * power[:, lanes]).astype(jnp.bfloat16)
            places = pl.ds(start * per_line + at, BLOCK_ROWS, stride=per_line)
            weighted_ref[places, :] = value.astype(jnp.float32)

    bins = bins_ref[...]
    high_ref[...] = (bins // LOW_BINS).astype(jnp.float32)
    low_ref[...] = (bins % LOW_BINS).astype(jnp.float32)
    high_index = lax.broadcasted_iota(jnp.int32, (HIGH_BINS, LANES), 0)
    high_index = high_index.astype(jnp.float32).astype(jnp.bfloat16)
    low_index = lax.broadcasted_iota(jnp.int32, (LOW_BINS, LANES), 0)
    low_index = low_index.astype(jnp.float32).astype(jnp.bfloat16)
    one, zero = (jnp.bfloat16(1.0), jnp.bfloat16(0.0))

    def step(at, total):
        start = at * STEP_LINES
        left, right = ([], [])

        def spread(block, line, count):
            return jnp.broadcast_to(block[line : line + 1], (count, LANES)).astype(jnp.bfloat16)

        lines_here = pl.ds(start, STEP_LINES)
        highs, lows, values = (high_ref[lines_here], low_ref[lines_here], weighted_ref[lines_here])
        for line in range(STEP_LINES):
            left.append(jnp.where(high_index == spread(highs, line, HIGH_BINS), one, zero))
            value = spread(values, line, LOW_BINS)
            right.append(jnp.where(low_index == spread(lows, line, LOW_BINS), value, zero))
        return total + lax.dot_general(
            jnp.concatenate(left, axis=1),
            jnp.concatenate(right, axis=1),
            ((((1,), (1,))), ((), ())),
            preferred_element_type=jnp.float32,
        )

    total = jnp.zeros((HIGH_BINS, LOW_BINS), jnp.float32)
    for at in range(HALF_ROWS * per_line // STEP_LINES):
        total = step(at, total)
    per_row = LANES // LOW_BINS
    total = jnp.concatenate([total, jnp.zeros((HIGH_BINS, LANES - LOW_BINS), jnp.float32)], axis=1)
    place = lax.broadcasted_iota(jnp.int32, (HIGH_BINS, LANES), 0) % per_row
    moved = jnp.where(place == 0, total, 0.0)
    for at in range(1, per_row):
        moved = moved + jnp.where(place == at, pltpu.roll(total, at * LOW_BINS, 1), 0.0)
    lines = BINS // LANES // shards
    for line in range(BINS // LANES):
        send_ref[line // lines, line % lines : line % lines + 1] = jnp.sum(
            moved[line * per_row : (line + 1) * per_row], axis=0, keepdims=True
        )
    pl.semaphore_wait(barrier, everyone - 1)

    def outgoing(index):
        return pltpu.make_async_remote_copy(
            src_ref=send_ref.at[lax.rem(index, shards)], dst_ref=recv_ref.at[here],
            send_sem=sems.at[0, index], recv_sem=sems.at[1, here],
            device_id=target(index), device_id_type=MESH,
        )

    def incoming(index):
        return pltpu.make_async_remote_copy(
            src_ref=send_ref.at[lax.rem(index, shards)], dst_ref=recv_ref.at[index],
            send_sem=sems.at[0, index], recv_sem=sems.at[1, index],
            device_id=target(index), device_id_type=MESH,
        )

    def begin(step, carry):
        outgoing(lax.rem(here + step, everyone)).start()
        return carry

    def arrive(step, carry):
        incoming(lax.rem(here + everyone - step, everyone)).wait_recv()
        return carry

    def leave(step, carry):
        outgoing(lax.rem(here + step, everyone)).wait_send()
        return carry

    lax.fori_loop(1, everyone, begin, 0)
    recv_ref[here] = send_ref[lax.axis_index("tm")]
    lax.fori_loop(1, everyone, arrive, 0)
    scale = BINS / (HALF_ROWS * COLS * shards)
    band = None
    mine = lax.axis_index("chan")
    for chan in range(chans):
        line = recv_ref[chan * shards]
        for at in range(1, shards):
            line = line + recv_ref[chan * shards + at]
        line = line * scale
        own = jnp.where(mine == chan, line, 0.0)
        band, profile = (line, own) if band is None else (band + line, profile + own)
    small_ref[0:lines] = profile
    small_ref[lines : 2 * lines] = band
    small_ref[2 * lines : 2 * lines + 1] = weight_row
    lax.fori_loop(1, everyone, leave, 0)


def fold(data, reply, flags, bins, chans, shards):
    vmem = pl.BlockSpec(memory_space=pltpu.VMEM)
    tables = (dft_table(), twiddle(), half_turns())
    lines = BINS // LANES // shards
    return pl.pallas_call(
        functools.partial(fold_kernel, chans, shards),
        out_shape=(
            jax.ShapeDtypeStruct((2, HALF_ROWS, COLS), jnp.bfloat16),
            jax.ShapeDtypeStruct((2 * lines + 1, LANES), jnp.float32),
        ),
        in_specs=[vmem] * 7,
        out_specs=(vmem,) * 2,
        scratch_shapes=[
            pltpu.VMEM((2, 2, 2, HALF_ROWS, COLS), jnp.bfloat16),
            pltpu.VMEM((HALF_ROWS * COLS // LANES, LANES), jnp.float32),
            pltpu.VMEM((HALF_ROWS * COLS // LANES, LANES), jnp.float32),
            pltpu.VMEM((HALF_ROWS * COLS // LANES, LANES), jnp.float32),
            pltpu.VMEM((shards, lines, LANES), jnp.float32),
            pltpu.VMEM((chans * shards, lines, LANES), jnp.float32),
            pltpu.SemaphoreType.DMA((2, chans * shards)),
        ],
        compiler_params=pltpu.CompilerParams(
            vmem_limit_bytes=40 << 20, collective_id=1, has_side_effects=True
        ),
        cost_estimate=pl.CostEstimate(
            flops=6 * 10**9, bytes_accessed=6 << 20, transcendentals=0
        ),
        name="fold",
    )(data, reply, flags, bins, *[jnp.asarray(table) for table in tables])


def on_device(voltages, antenna_gains, chirp_phase, offsets, flags, sample_phase_bins):
    shards, chans = (lax.axis_size("tm"), lax.axis_size("chan"))
    antennas, channels, samples = voltages.shape[1:]
    assert channels == 1 and shards % 2 == 0
    volts = voltages.reshape(2, antennas, samples // LANES, LANES)
    volts = jnp.transpose(volts, (0, 2, 1, 3)).reshape(2, samples // LANES * antennas, LANES)
    gains = jnp.transpose(antenna_gains, (0, 2, 1))
    data, reply = beam(volts, gains, offsets, chirp_phase.reshape(-1, LANES), shards)
    bins = sample_phase_bins.reshape(-1, LANES)
    dedispersed, small = fold(data, reply, flags, bins, chans, shards)
    lines = BINS // LANES // shards
    return (
        dedispersed.reshape(2, 1, HALF_ROWS * COLS),
        small[2 * lines : 2 * lines + 1, :WINDOWS],
        small[:lines].reshape(1, BINS // shards),
        small[lines : 2 * lines].reshape(BINS // shards),
    )


def solution(mesh):
    placed = (
        P(None, "tm", "chan", None),
        P(None, None, "chan"),
        P("chan", None),
        P("chan"),
        P("chan", "tm"),
        P("tm"),
    )
    return jax.shard_map(
        on_device,
        mesh=mesh,
        in_specs=placed,
        out_specs=(P(None, "chan", "tm"), P("chan", "tm"), P("chan", "tm"), P("tm")),
        check_vma=False,
    )
```

```python
import functools
import math

import jax
import jax.numpy as jnp
import numpy as np
from jax import lax
from jax.experimental import pallas as pl
from jax.experimental.pallas import tpu as pltpu
from jax.sharding import PartitionSpec as P

NFFT = 131072
OFFSET_BOUND = 4096
SKW = 1024
BINS = 2048


SK_WIDTH = 0.05
EPSILON = 1e-06

COLS = 1 << (NFFT.bit_length() - 1) // 2
ROWS = NFFT // COLS
HALF_ROWS = ROWS // 2
HALO_ROWS = OFFSET_BOUND // COLS
WIN_ROWS = SKW // COLS
WINDOWS = HALF_ROWS // WIN_ROWS
LOW_BINS = 32
HIGH_BINS = BINS // LOW_BINS
BLOCK_ROWS = 128
STEP_LINES = 8
LANES = 128
DEPTH = 256
PARTS = 4
PART_ROWS = HALF_ROWS // PARTS
MESH = pl.DeviceIdType.MESH


def bf16_split(table):
    high = table.astype(jnp.bfloat16)
    low = (table - high.astype(np.float32)).astype(jnp.bfloat16)
    return np.stack([high, low])


def unit_roots(turns, period):
    angle = -2.0 * math.pi / period * (turns % period)
    return (np.cos(angle).astype(np.float32), np.sin(angle).astype(np.float32))


def dft_table():
    index = np.arange(COLS, dtype=np.int64)
    real, imag = unit_roots(index[:, None] * index[None, :], COLS)
    return bf16_split(np.concatenate([-imag, real, imag]))


def twiddle():
    index = np.arange(HALF_ROWS, dtype=np.int64)
    rows = np.stack([2 * index, 2 * index + 1])
    return np.stack(unit_roots(rows[:, :, None] * np.arange(COLS, dtype=np.int64), NFFT))


def half_turns():
    index = np.arange(HALF_ROWS, dtype=np.int64)
    return np.stack(unit_roots(np.repeat(index[:, None], LANES, axis=1), ROWS))


def split(value):
    high = value.astype(jnp.bfloat16)
    return high, (value - high.astype(jnp.float32)).astype(jnp.bfloat16)


def product(*pairs):
    left, right = ([], [])
    for a, b in pairs:
        left += [a[0], a[0], a[1]]
        right += [b[0], b[1], b[0]]
    return jnp.dot(
        jnp.concatenate(left, axis=1),
        jnp.concatenate(right, axis=0),
        preferred_element_type=jnp.float32,
    )


def cos_sin(angle):
    half = 0.5 * angle
    square = half * half
    sine = jnp.full_like(square, 1.0 / math.factorial(13))
    for power in (11, 9, 7, 5, 3, 1):
        sine = sine * square + (-1.0) ** (power // 2) / math.factorial(power)
    sine = sine * half
    cosine = jnp.full_like(square, 1.0 / math.factorial(12))
    for power in (10, 8, 6, 4, 2, 0):
        cosine = cosine * square + (-1.0) ** (power // 2) / math.factorial(power)
    return 1.0 - 2.0 * sine * sine, 2.0 * sine * cosine


def response(phase, first, first_column, offset):
    index = first + lax.broadcasted_iota(jnp.int32, phase.shape, 0)
    column = first_column + lax.broadcasted_iota(jnp.int32, phase.shape, 1)
    index = index + ROWS * column
    turns = (index * offset) & (NFFT - 1)
    turns = jnp.where(turns >= NFFT // 2, turns - NFFT, turns)
    phase = phase + turns.astype(jnp.float32) * (2.0 * math.pi / NFFT)
    phase = jnp.where(phase > math.pi, phase - 2.0 * math.pi, phase)
    phase = jnp.where(phase < -math.pi, phase + 2.0 * math.pi, phase)
    return cos_sin(phase)


def weight_table(gains_ref, table_ref, antennas, me):
    total = gains_ref.shape[2]
    lane = lax.broadcasted_iota(jnp.int32, (8, LANES), 1)
    wide = []
    for part in range(2):
        row = gains_ref[part]
        if total < LANES:
            row = jnp.concatenate([row, jnp.zeros((1, LANES - total), jnp.float32)], axis=1)
        row = jnp.broadcast_to(row, (8, LANES))
        row = pltpu.roll(row, lax.rem(LANES - me * antennas, LANES), 1)
        row = jnp.where(lane < antennas, row, 0.0)
        width = antennas
        while width < LANES:
            row = row + pltpu.roll(row, width, 1)
            width *= 2
        wide.append(jnp.concatenate([row] * (DEPTH // LANES), axis=1)[:1])
    real, imag = wide
    half = DEPTH // antennas // 2
    shape = (half, DEPTH)
    tile = lax.broadcasted_iota(jnp.int32, shape, 1) // antennas
    index = lax.broadcasted_iota(jnp.int32, shape, 0)
    for source, pair in enumerate(((real, imag), (-imag, real))):
        for out, values in enumerate(pair):
            for parity in range(2):
                dense = jnp.where(tile == 2 * index + parity, values, 0.0)
                high, low = split(dense)
                at = (2 * out + parity) * half
                table_ref[source, at : at + half] = high
                table_ref[source, 4 * half + at : 4 * half + at + half] = low


def part_beam(table_ref, volt_ref, antennas, put):
    half = DEPTH // antennas // 2
    groups = volt_ref.shape[1] // DEPTH
    joined = 2 if groups % 2 == 0 else 1
    for at in range(groups // joined):
        total = None
        for source in range(2):
            lanes = [
                volt_ref[source, (joined * at + b) * DEPTH : (joined * at + b + 1) * DEPTH]
                for b in range(joined)
            ]
            right = lanes[0] if joined == 1 else jnp.concatenate(lanes, axis=1)
            term = jnp.dot(table_ref[source], right, preferred_element_type=jnp.float32)
            total = term if total is None else total + term
        total = total[: 4 * half] + total[4 * half :]
        for b in range(joined):
            block = total[:, b * LANES : (b + 1) * LANES]
            for out in range(2):
                even = block[2 * out * half : (2 * out + 1) * half]
                odd = block[(2 * out + 1) * half : (2 * out + 2) * half]
                put(out, (joined * at + b) * half, half, jnp.concatenate([even, odd], axis=1))


def beam_kernel(
    antennas, pairs, volt_ref, gains_hbm, offset_ref, chirp_hbm, turns_hbm, data_ref, response_ref,
    table_ref, vbuf, pair_send, pair_recv, chip_send, chip_recv, own_ref, halo_send, halo_ref,
    head_ref, gains_ref, chirp_ref, turns_ref, block_ref, load_sem, pair_sems, chip_sems, halo_sems,
    head_sems, side_sems,
):
    count = 2 * pairs
    me = lax.axis_index("tm")
    pair, core = (me // 2, lax.rem(me, 2))
    barrier = pltpu.get_barrier_semaphore()
    for step in range(1, count):
        pl.semaphore_signal(
            barrier, inc=1, device_id={"tm": lax.rem(me + step, count)}, device_id_type=MESH
        )
    size = vbuf.shape[3]

    def shard_of(j, other):
        return lax.rem(pair + 1 + j, pairs) * 2 + (1 - core if other else core)

    def load(part, j, other):
        start = pl.multiple_of((shard_of(j, other) * PARTS + part) * size, size)
        slot = 2 * j + (0 if other else 1)
        return pltpu.make_async_copy(
            volt_ref.at[:, pl.ds(start, size)], vbuf.at[part, slot], load_sem.at[part, slot]
        )

    def order():
        return [(j, True) for j in range(pairs)] + [(j, False) for j in range(pairs)]

    def begin(part, carry):
        for j, other in order():
            load(part, j, other).start()
        return carry

    gains_copy = pltpu.make_async_copy(gains_hbm, gains_ref, side_sems.at[2])
    gains_copy.start()
    lax.fori_loop(0, PARTS, begin, 0)
    side = [
        pltpu.make_async_copy(chirp_hbm, chirp_ref, side_sems.at[0]),
        pltpu.make_async_copy(turns_hbm, turns_ref, side_sems.at[1]),
    ]
    for copy in side:
        copy.start()
    offset = offset_ref[0]
    gains_copy.wait()
    weight_table(gains_ref, table_ref, antennas, me)

    def pair_copy(part, j):
        return pltpu.make_async_remote_copy(
            src_ref=pair_send.at[part, j], dst_ref=pair_recv.at[part, j],
            send_sem=pair_sems.at[0, part, j], recv_sem=pair_sems.at[1, part, j],
            device_id={"tm": pair * 2 + (1 - core)}, device_id_type=MESH,
        )

    def chip_copy(part, j):
        return pltpu.make_async_remote_copy(
            src_ref=chip_send.at[part, j], dst_ref=chip_recv.at[part, j],
            send_sem=chip_sems.at[0, part, j], recv_sem=chip_sems.at[1, part, j],
            device_id={"tm": shard_of(j, False)}, device_id_type=MESH,
        )

    def halo_copy(part):
        return pltpu.make_async_remote_copy(
            src_ref=halo_send.at[part], dst_ref=halo_ref.at[part],
            send_sem=halo_sems.at[0, part], recv_sem=halo_sems.at[1, part],
            device_id={"tm": lax.rem(me + 1, count)}, device_id_type=MESH,
        )

    def head_copy():
        return pltpu.make_async_remote_copy(
            src_ref=halo_send.at[0, :, 0:HALO_ROWS], dst_ref=head_ref,
            send_sem=head_sems.at[0], recv_sem=head_sems.at[1],
            device_id={"tm": lax.rem(me + count - 1, count)}, device_id_type=MESH,
        )

    def finish(part):
        for j in range(pairs - 1):
            chip_copy(part, j).wait_recv()
        total = own_ref[part]
        for j in range(pairs - 1):
            total = total + chip_recv[part, j].astype(jnp.float32)
        own_ref[part] = total
        halo_send[part] = total.astype(jnp.bfloat16)

        @pl.when(me < count - 1)
        def _():
            halo_copy(part).start()

    def chirp_block(at):
        stride = ROWS // LANES
        for half in range(COLS // LANES):
            columns = chirp_ref[
                pl.ds(at + half * LANES * stride, LANES, stride=stride), :
            ]
            phase = jnp.transpose(columns, (1, 0))
            for out, value in enumerate(response(phase, at * LANES, half * LANES, offset)):
                block_ref[...] = value * (1.0 / NFFT)
                for parity in range(2):
                    rows = pl.ds(pl.multiple_of(at * (LANES // 2), LANES // 2), LANES // 2)
                    response_ref[out, parity, rows, half * LANES : (half + 1) * LANES] = (
                        block_ref[pl.ds(parity, LANES // 2, stride=2), :]
                    )

    def combine(part, first=None):
        rows = slice(part * PART_ROWS, (part + 1) * PART_ROWS)
        before = [halo_ref[part, out].astype(jnp.float32) for out in range(2)]
        if first is not None:
            before = [
                jnp.concatenate([head, value[HALO_ROWS:]], axis=0)
                for head, value in zip(first, before)
            ]
        after = [own_ref[part, 0], own_ref[part, 1]]
        real, imag = (before[0] - after[0], before[1] - after[1])
        cosine, sine = [
            jnp.concatenate([turns_ref[out, rows]] * (COLS // LANES), axis=1) for out in range(2)
        ]
        both = (
            (before[0] + after[0], before[1] + after[1]),
            (real * cosine - imag * sine, real * sine + imag * cosine),
        )
        for kind, values in enumerate(both):
            for out, value in enumerate(values):
                data_ref[kind, out, 0, rows], data_ref[kind, out, 1, rows] = split(value)

    def run(part, carry):
        for j in range(pairs):
            load(part, j, True).wait()

            def put(out, at, rows, value, j=j):
                pair_send[part, j, out, at : at + rows] = value

            part_beam(table_ref, vbuf.at[part, 2 * j], antennas, put)
            if j == 0:

                @pl.when(part == 0)
                def _():
                    pl.semaphore_wait(barrier, count - 1)

            pair_copy(part, j).start()
        for j in range(pairs):
            load(part, j, False).wait()
            pair_copy(part, j).wait_recv()
            if j < pairs - 1:

                def put(out, at, rows, value, j=j):
                    value = value + pair_recv[part, j, out, at : at + rows]
                    chip_send[part, j, out, at : at + rows] = value.astype(jnp.bfloat16)

            else:

                def put(out, at, rows, value, j=j):
                    value = value + pair_recv[part, j, out, at : at + rows]
                    own_ref[part, out, at : at + rows] = value

            part_beam(table_ref, vbuf.at[part, 2 * j + 1], antennas, put)
            if j < pairs - 1:
                chip_copy(part, j).start()

        @pl.when(part == 0)
        def _():
            for copy in side:
                copy.wait()

        chirp_block(part)

        @pl.when(part > 0)
        def _():
            finish(part - 1)

            @pl.when((part == 1) & (me > 0))
            def _():
                head_copy().start()

        return carry

    lax.fori_loop(0, PARTS, run, 0)
    finish(PARTS - 1)

    @pl.when(me == 0)
    def _():
        halo_ref[...] = jnp.zeros((PARTS, 2, PART_ROWS, COLS), jnp.bfloat16)

    @pl.when(me == count - 1)
    def _():
        head_ref[...] = jnp.zeros((2, HALO_ROWS, COLS), jnp.bfloat16)

    for part in range(PARTS):

        @pl.when(me > 0)
        def _():
            halo_copy(part).wait_recv()

        first = None
        if part == 0:

            @pl.when(me < count - 1)
            def _():
                head_copy().wait_recv()

            spot = lax.broadcasted_iota(jnp.int32, (HALO_ROWS, COLS), 0) * COLS
            spot = spot + lax.broadcasted_iota(jnp.int32, (HALO_ROWS, COLS), 1)
            first = [
                jnp.where(
                    spot < offset,
                    head_ref[out].astype(jnp.float32),
                    halo_ref[0, out, 0:HALO_ROWS].astype(jnp.float32),
                )
                for out in range(2)
            ]
        combine(part, first)

    @pl.when(me > 0)
    def _():
        head_copy().wait_send()

    @pl.when(me < count - 1)
    def _():
        for part in range(PARTS):
            halo_copy(part).wait_send()

    def drain(part, carry):
        for j in range(pairs):
            pair_copy(part, j).wait_send()
            if j < pairs - 1:
                chip_copy(part, j).wait_send()
        return carry

    lax.fori_loop(0, PARTS, drain, 0)


def beam(volts, gains, offset, chirp, shards):
    pairs = shards // 2
    size = volts.shape[1] // shards // PARTS
    antennas = size * LANES // (PART_ROWS * COLS)
    half = DEPTH // antennas // 2
    block = (2, PART_ROWS, COLS)
    vmem = pl.BlockSpec(memory_space=pltpu.VMEM)
    hbm = pl.BlockSpec(memory_space=pltpu.HBM)
    keep = functools.partial(pltpu.with_memory_space_constraint, memory_space=pltpu.HBM)
    return pl.pallas_call(
        functools.partial(beam_kernel, antennas, pairs),
        out_shape=(
            jax.ShapeDtypeStruct((2, 2, 2, HALF_ROWS, COLS), jnp.bfloat16),
            jax.ShapeDtypeStruct((2, 2, HALF_ROWS, COLS), jnp.float32),
        ),
        in_specs=[hbm, hbm, pl.BlockSpec(memory_space=pltpu.SMEM), hbm, hbm],
        out_specs=(vmem, vmem),
        scratch_shapes=[
            pltpu.VMEM((2, 8 * half, DEPTH), jnp.bfloat16),
            pltpu.VMEM((PARTS, shards, 2, size, LANES), jnp.bfloat16),
            pltpu.VMEM((PARTS, pairs) + block, jnp.float32),
            pltpu.VMEM((PARTS, pairs) + block, jnp.float32),
            pltpu.VMEM((PARTS, pairs - 1) + block, jnp.bfloat16),
            pltpu.VMEM((PARTS, pairs - 1) + block, jnp.bfloat16),
            pltpu.VMEM((PARTS,) + block, jnp.float32),
            pltpu.VMEM((PARTS,) + block, jnp.bfloat16),
            pltpu.VMEM((PARTS,) + block, jnp.bfloat16),
            pltpu.VMEM((2, HALO_ROWS, COLS), jnp.bfloat16),
            pltpu.VMEM(gains.shape, jnp.float32),
            pltpu.VMEM((NFFT // LANES, LANES), jnp.float32),
            pltpu.VMEM((2, HALF_ROWS, LANES), jnp.float32),
            pltpu.VMEM((LANES, LANES), jnp.float32),
            pltpu.SemaphoreType.DMA((PARTS, shards)),
            pltpu.SemaphoreType.DMA((2, PARTS, pairs)),
            pltpu.SemaphoreType.DMA((2, PARTS, pairs - 1)),
            pltpu.SemaphoreType.DMA((2, PARTS)),
            pltpu.SemaphoreType.DMA((2,)),
            pltpu.SemaphoreType.DMA((3,)),
        ],
        compiler_params=pltpu.CompilerParams(
            vmem_limit_bytes=44 << 20, collective_id=0, has_side_effects=True
        ),
        cost_estimate=pl.CostEstimate(
            flops=3 * 10**9, bytes_accessed=18 << 20, transcendentals=0
        ),
        name="beam",
    )(keep(volts), keep(gains), offset, keep(chirp), keep(jnp.asarray(half_turns())))


def fold_kernel(
    chans, shards, data_ref, response_ref, flags_ref, bins_ref, dft_ref, twist_ref, turns_ref,
    dedispersed_ref, small_ref, weighted_ref, high_ref, low_ref, send_ref, recv_ref,
    sems,
):
    everyone = chans * shards
    here = lax.axis_index("chan") * shards + lax.axis_index("tm")
    barrier = pltpu.get_barrier_semaphore()

    def target(index):
        return {"chan": index // shards, "tm": lax.rem(index, shards)}

    def greet(step, carry):
        pl.semaphore_signal(
            barrier, inc=1, device_id=target(lax.rem(here + step, everyone)), device_id_type=MESH
        )
        return carry

    lax.fori_loop(1, everyone, greet, 0)
    def table(start, count=1):
        rows = slice(start * COLS, (start + count) * COLS)
        return (dft_ref[0, rows], dft_ref[1, rows])

    minus_table, real_table, imag_table = (table(0), table(1), table(2))
    forward, cross = (table(1, 2), table(0, 2))
    pairs = []
    for kind in range(2):
        given = [(data_ref[kind, out, 0], data_ref[kind, out, 1]) for out in range(2)]
        both = product((forward, given[0]), (cross, given[1]))
        pairs.append((both[:HALF_ROWS], both[HALF_ROWS:]))
    for kind in range(2):
        real, imag = pairs[kind]
        cosine, sine = (twist_ref[0, kind], twist_ref[1, kind])
        pairs[kind] = (split(real * cosine - imag * sine), split(real * sine + imag * cosine))
    for kind in range(2):
        real, imag = pairs[kind]
        pairs[kind] = (
            product((real, real_table), (imag, minus_table)),
            product((real, imag_table), (imag, real_table)),
        )
    for kind in range(2):
        real, imag = pairs[kind]
        turn, tilt = (response_ref[0, kind], response_ref[1, kind])
        pairs[kind] = (split(real * turn - imag * tilt), split(real * tilt + imag * turn))
    for kind in range(2):
        real, imag = pairs[kind]
        pairs[kind] = (
            product((real, real_table), (imag, imag_table)),
            product((real, minus_table), (imag, real_table)),
        )
    for kind in range(2):
        real, imag = pairs[kind]
        cosine, sine = (twist_ref[0, kind], twist_ref[1, kind])
        pairs[kind] = (split(real * cosine + imag * sine), split(imag * cosine - real * sine))
    for kind in range(2):
        real, imag = pairs[kind]
        both = product((cross, real), (forward, imag))
        pairs[kind] = (both[HALF_ROWS:], both[:HALF_ROWS])

    flag = flags_ref[...]
    if WINDOWS < LANES:
        flag = jnp.concatenate([flag, jnp.zeros((1, LANES - WINDOWS), jnp.int32)], axis=1)
    keep_row = (1 - flag).astype(jnp.float32)
    shape = (BLOCK_ROWS, LANES)
    row_index = lax.broadcasted_iota(jnp.int32, shape, 0)
    lane_index = lax.broadcasted_iota(jnp.int32, shape, 1)

    def window_sum(values):
        total = jnp.broadcast_to(jnp.sum(values, axis=1, keepdims=True), shape)
        reach = 1
        while reach < WIN_ROWS:
            up, down = (pltpu.roll(total, BLOCK_ROWS - reach, 0), pltpu.roll(total, reach, 0))
            total = total + jnp.where(row_index % (2 * reach) < reach, up, down)
            reach *= 2
        return total

    per_line = COLS // LANES
    weight_row = jnp.zeros((1, LANES), jnp.float32)
    for start in range(0, HALF_ROWS, BLOCK_ROWS):
        rows = slice(start, start + BLOCK_ROWS)
        cosine, sine = [
            jnp.concatenate([turns_ref[out, rows]] * (COLS // LANES), axis=1) for out in range(2)
        ]
        (real, imag), (odd_real, odd_imag) = [[value[rows] for value in pair] for pair in pairs]
        real = real - (odd_real * cosine + odd_imag * sine)
        imag = imag - (odd_imag * cosine - odd_real * sine)
        dedispersed_ref[0, rows] = real.astype(jnp.bfloat16)
        dedispersed_ref[1, rows] = imag.astype(jnp.bfloat16)
        power = real * real + imag * imag
        first_sum, second_sum = (window_sum(power), window_sum(power * power))
        kurtosis = (
            (SKW + 1.0)
            / (SKW - 1.0)
            * (SKW * second_sum / (first_sum * first_sum + EPSILON) - 1.0)
        )
        scaled = (kurtosis - 1.0) / SK_WIDTH
        window = (row_index + start) // WIN_ROWS
        keep = jnp.where(lane_index == window, jnp.broadcast_to(keep_row, shape), 0.0)
        keep = jnp.sum(keep, axis=1, keepdims=True)
        sk_weight = keep / (1.0 + scaled * scaled)
        chosen = (row_index + start) == lane_index * WIN_ROWS
        weight_row = weight_row + jnp.sum(
            jnp.where(chosen, sk_weight, 0.0), axis=0, keepdims=True
        )
        for at in range(COLS // LANES):
            lanes = slice(at * LANES, (at + 1) * LANES)
            value = (sk_weight * power[:, lanes]).astype(jnp.bfloat16)
            places = pl.ds(start * per_line + at, BLOCK_ROWS, stride=per_line)
            weighted_ref[places, :] = value.astype(jnp.float32)

    bins = bins_ref[...]
    high_ref[...] = (bins // LOW_BINS).astype(jnp.float32)
    low_ref[...] = (bins % LOW_BINS).astype(jnp.float32)
    high_index = lax.broadcasted_iota(jnp.int32, (HIGH_BINS, LANES), 0)
    high_index = high_index.astype(jnp.float32).astype(jnp.bfloat16)
    low_index = lax.broadcasted_iota(jnp.int32, (LOW_BINS, LANES), 0)
    low_index = low_index.astype(jnp.float32).astype(jnp.bfloat16)
    minus, zero = (jnp.bfloat16(-1.0), jnp.bfloat16(0.0))

    def step(at, total):
        start = at * STEP_LINES
        left, right = ([], [])

        def spread(block, line, count):
            return jnp.broadcast_to(block[line : line + 1], (count, LANES)).astype(jnp.bfloat16)

        lines_here = pl.ds(start, STEP_LINES)
        highs, lows, values = (high_ref[lines_here], low_ref[lines_here], weighted_ref[lines_here])
        for line in range(STEP_LINES):
            left.append(jnp.where(high_index == spread(highs, line, HIGH_BINS), minus, zero))
            value = spread(values, line, LOW_BINS)
            right.append(jnp.where(low_index == spread(lows, line, LOW_BINS), value, zero))
        return total - lax.dot_general(
            jnp.concatenate(left, axis=1),
            jnp.concatenate(right, axis=1),
            ((((1,), (1,))), ((), ())),
            preferred_element_type=jnp.float32,
        )

    totals = [jnp.zeros((HIGH_BINS, LOW_BINS), jnp.float32)] * 2
    for at in range(HALF_ROWS * per_line // STEP_LINES):
        totals[at % 2] = step(at, totals[at % 2])
    total = totals[0] + totals[1]
    per_row = LANES // LOW_BINS
    total = jnp.concatenate([total, jnp.zeros((HIGH_BINS, LANES - LOW_BINS), jnp.float32)], axis=1)
    place = lax.broadcasted_iota(jnp.int32, (HIGH_BINS, LANES), 0) % per_row
    moved = jnp.where(place == 0, total, 0.0)
    for at in range(1, per_row):
        moved = moved + jnp.where(place == at, pltpu.roll(total, at * LOW_BINS, 1), 0.0)
    lines = BINS // LANES // shards
    for line in range(BINS // LANES):
        send_ref[line // lines, line % lines : line % lines + 1] = jnp.sum(
            moved[line * per_row : (line + 1) * per_row], axis=0, keepdims=True
        )
    pl.semaphore_wait(barrier, everyone - 1)

    def outgoing(index):
        return pltpu.make_async_remote_copy(
            src_ref=send_ref.at[lax.rem(index, shards)], dst_ref=recv_ref.at[here],
            send_sem=sems.at[0, index], recv_sem=sems.at[1, here],
            device_id=target(index), device_id_type=MESH,
        )

    def incoming(index):
        return pltpu.make_async_remote_copy(
            src_ref=send_ref.at[lax.rem(index, shards)], dst_ref=recv_ref.at[index],
            send_sem=sems.at[0, index], recv_sem=sems.at[1, index],
            device_id=target(index), device_id_type=MESH,
        )

    def begin(step, carry):
        outgoing(lax.rem(here + step, everyone)).start()
        return carry

    def arrive(step, carry):
        incoming(lax.rem(here + everyone - step, everyone)).wait_recv()
        return carry

    def leave(step, carry):
        outgoing(lax.rem(here + step, everyone)).wait_send()
        return carry

    lax.fori_loop(1, everyone, begin, 0)
    recv_ref[here] = send_ref[lax.axis_index("tm")]
    lax.fori_loop(1, everyone, arrive, 0)
    scale = BINS / (HALF_ROWS * COLS * shards)
    band = None
    mine = lax.axis_index("chan")
    for chan in range(chans):
        line = recv_ref[chan * shards]
        for at in range(1, shards):
            line = line + recv_ref[chan * shards + at]
        line = line * scale
        own = jnp.where(mine == chan, line, 0.0)
        band, profile = (line, own) if band is None else (band + line, profile + own)
    small_ref[0:lines] = profile
    small_ref[lines : 2 * lines] = band
    small_ref[2 * lines : 2 * lines + 1] = weight_row
    lax.fori_loop(1, everyone, leave, 0)


def fold(data, reply, flags, bins, chans, shards):
    vmem = pl.BlockSpec(memory_space=pltpu.VMEM)
    tables = (dft_table(), twiddle(), half_turns())
    lines = BINS // LANES // shards
    return pl.pallas_call(
        functools.partial(fold_kernel, chans, shards),
        out_shape=(
            jax.ShapeDtypeStruct((2, HALF_ROWS, COLS), jnp.bfloat16),
            jax.ShapeDtypeStruct((2 * lines + 1, LANES), jnp.float32),
        ),
        in_specs=[vmem] * 7,
        out_specs=(vmem,) * 2,
        scratch_shapes=[
            pltpu.VMEM((HALF_ROWS * COLS // LANES, LANES), jnp.float32),
            pltpu.VMEM((HALF_ROWS * COLS // LANES, LANES), jnp.float32),
            pltpu.VMEM((HALF_ROWS * COLS // LANES, LANES), jnp.float32),
            pltpu.VMEM((shards, lines, LANES), jnp.float32),
            pltpu.VMEM((chans * shards, lines, LANES), jnp.float32),
            pltpu.SemaphoreType.DMA((2, chans * shards)),
        ],
        compiler_params=pltpu.CompilerParams(
            vmem_limit_bytes=40 << 20, collective_id=1, has_side_effects=True
        ),
        cost_estimate=pl.CostEstimate(
            flops=6 * 10**9, bytes_accessed=6 << 20, transcendentals=0
        ),
        name="fold",
    )(data, reply, flags, bins, *[jnp.asarray(table) for table in tables])


def on_device(voltages, antenna_gains, chirp_phase, offsets, flags, sample_phase_bins):
    shards, chans = (lax.axis_size("tm"), lax.axis_size("chan"))
    antennas, channels, samples = voltages.shape[1:]
    assert channels == 1 and shards % 2 == 0
    volts = voltages.reshape(2, antennas, samples // LANES, LANES)
    volts = jnp.transpose(volts, (0, 2, 1, 3)).reshape(2, samples // LANES * antennas, LANES)
    gains = jnp.transpose(antenna_gains, (0, 2, 1))
    data, reply = beam(volts, gains, offsets, chirp_phase.reshape(-1, LANES), shards)
    bins = sample_phase_bins.reshape(-1, LANES)
    dedispersed, small = fold(data, reply, flags, bins, chans, shards)
    lines = BINS // LANES // shards
    return (
        dedispersed.reshape(2, 1, HALF_ROWS * COLS),
        small[2 * lines : 2 * lines + 1, :WINDOWS],
        small[:lines].reshape(1, BINS // shards),
        small[lines : 2 * lines].reshape(BINS // shards),
    )


def solution(mesh):
    placed = (
        P(None, "tm", "chan", None),
        P(None, None, "chan"),
        P("chan", None),
        P("chan"),
        P("chan", "tm"),
        P("tm"),
    )
    return jax.shard_map(
        on_device,
        mesh=mesh,
        in_specs=placed,
        out_specs=(P(None, "chan", "tm"), P("chan", "tm"), P("chan", "tm"), P("tm")),
        check_vma=False,
    )
```

```python
import functools
import math

import jax
import jax.numpy as jnp
import numpy as np
from jax import lax
from jax.experimental import pallas as pl
from jax.experimental.pallas import tpu as pltpu
from jax.sharding import PartitionSpec as P

NFFT = 131072
OFFSET_BOUND = 4096
SKW = 1024
BINS = 2048


SK_WIDTH = 0.05
EPSILON = 1e-06

COLS = 1 << (NFFT.bit_length() - 1) // 2
ROWS = NFFT // COLS
HALF_ROWS = ROWS // 2
HALO_ROWS = OFFSET_BOUND // COLS
WIN_ROWS = SKW // COLS
WINDOWS = HALF_ROWS // WIN_ROWS
LOW_BINS = 32
HIGH_BINS = BINS // LOW_BINS
BLOCK_ROWS = 128
STEP_LINES = 8
LANES = 128
DEPTH = 256
PARTS = 8
PART_ROWS = HALF_ROWS // PARTS
MESH = pl.DeviceIdType.MESH


def bf16_split(table):
    high = table.astype(jnp.bfloat16)
    low = (table - high.astype(np.float32)).astype(jnp.bfloat16)
    return np.stack([high, low])


def unit_roots(turns, period):
    angle = -2.0 * math.pi / period * (turns % period)
    return (np.cos(angle).astype(np.float32), np.sin(angle).astype(np.float32))


def dft_table():
    index = np.arange(COLS, dtype=np.int64)
    real, imag = unit_roots(index[:, None] * index[None, :], COLS)
    return bf16_split(np.concatenate([-imag, real, imag]))


def twiddle():
    index = np.arange(HALF_ROWS, dtype=np.int64)
    rows = np.stack([2 * index, 2 * index + 1])
    return np.stack(unit_roots(rows[:, :, None] * np.arange(COLS, dtype=np.int64), NFFT))


def half_turns():
    index = np.arange(HALF_ROWS, dtype=np.int64)
    return np.stack(unit_roots(np.repeat(index[:, None], LANES, axis=1), ROWS))


def split(value):
    high = value.astype(jnp.bfloat16)
    return high, (value - high.astype(jnp.float32)).astype(jnp.bfloat16)


def product(*pairs):
    left, right = ([], [])
    for a, b in pairs:
        left += [a[0], a[0], a[1]]
        right += [b[0], b[1], b[0]]
    return jnp.dot(
        jnp.concatenate(left, axis=1),
        jnp.concatenate(right, axis=0),
        preferred_element_type=jnp.float32,
    )


def cos_sin(angle):
    half = 0.5 * angle
    square = half * half
    sine = jnp.full_like(square, 1.0 / math.factorial(13))
    for power in (11, 9, 7, 5, 3, 1):
        sine = sine * square + (-1.0) ** (power // 2) / math.factorial(power)
    sine = sine * half
    cosine = jnp.full_like(square, 1.0 / math.factorial(12))
    for power in (10, 8, 6, 4, 2, 0):
        cosine = cosine * square + (-1.0) ** (power // 2) / math.factorial(power)
    return 1.0 - 2.0 * sine * sine, 2.0 * sine * cosine


def response(phase, first, first_column, offset):
    index = first + lax.broadcasted_iota(jnp.int32, phase.shape, 0)
    column = first_column + lax.broadcasted_iota(jnp.int32, phase.shape, 1)
    index = index + ROWS * column
    turns = (index * offset) & (NFFT - 1)
    turns = jnp.where(turns >= NFFT // 2, turns - NFFT, turns)
    phase = phase + turns.astype(jnp.float32) * (2.0 * math.pi / NFFT)
    phase = jnp.where(phase > math.pi, phase - 2.0 * math.pi, phase)
    phase = jnp.where(phase < -math.pi, phase + 2.0 * math.pi, phase)
    return cos_sin(phase)


def weight_table(gains_ref, table_ref, antennas, me):
    total = gains_ref.shape[2]
    lane = lax.broadcasted_iota(jnp.int32, (8, LANES), 1)
    wide = []
    for part in range(2):
        row = gains_ref[part]
        if total < LANES:
            row = jnp.concatenate([row, jnp.zeros((1, LANES - total), jnp.float32)], axis=1)
        row = jnp.broadcast_to(row, (8, LANES))
        row = pltpu.roll(row, lax.rem(LANES - me * antennas, LANES), 1)
        row = jnp.where(lane < antennas, row, 0.0)
        width = antennas
        while width < LANES:
            row = row + pltpu.roll(row, width, 1)
            width *= 2
        wide.append(jnp.concatenate([row] * (DEPTH // LANES), axis=1)[:1])
    real, imag = wide
    half = DEPTH // antennas // 2
    shape = (half, DEPTH)
    tile = lax.broadcasted_iota(jnp.int32, shape, 1) // antennas
    index = lax.broadcasted_iota(jnp.int32, shape, 0)
    for source, pair in enumerate(((real, imag), (-imag, real))):
        for out, values in enumerate(pair):
            for parity in range(2):
                dense = jnp.where(tile == 2 * index + parity, values, 0.0)
                high, low = split(dense)
                at = (2 * out + parity) * half
                table_ref[source, at : at + half] = high
                table_ref[source, 4 * half + at : 4 * half + at + half] = low


def part_beam(table_ref, volt_ref, antennas, put):
    half = DEPTH // antennas // 2
    groups = volt_ref.shape[1] // DEPTH
    joined = 2 if groups % 2 == 0 else 1
    for at in range(groups // joined):
        total = None
        for source in range(2):
            lanes = [
                volt_ref[source, (joined * at + b) * DEPTH : (joined * at + b + 1) * DEPTH]
                for b in range(joined)
            ]
            right = lanes[0] if joined == 1 else jnp.concatenate(lanes, axis=1)
            term = jnp.dot(table_ref[source], right, preferred_element_type=jnp.float32)
            total = term if total is None else total + term
        total = total[: 4 * half] + total[4 * half :]
        for b in range(joined):
            block = total[:, b * LANES : (b + 1) * LANES]
            for out in range(2):
                even = block[2 * out * half : (2 * out + 1) * half]
                odd = block[(2 * out + 1) * half : (2 * out + 2) * half]
                put(out, (joined * at + b) * half, half, jnp.concatenate([even, odd], axis=1))


def beam_kernel(
    antennas, pairs, volt_ref, gains_hbm, offset_ref, chirp_hbm, turns_hbm, data_ref, response_ref,
    table_ref, vbuf, pair_send, pair_recv, chip_send, chip_recv, own_ref, halo_send, halo_ref,
    head_ref, gains_ref, chirp_ref, turns_ref, block_ref, load_sem, pair_sems, chip_sems, halo_sems,
    head_sems, side_sems,
):
    count = 2 * pairs
    me = lax.axis_index("tm")
    pair, core = (me // 2, lax.rem(me, 2))
    barrier = pltpu.get_barrier_semaphore()
    for step in range(1, count):
        pl.semaphore_signal(
            barrier, inc=1, device_id={"tm": lax.rem(me + step, count)}, device_id_type=MESH
        )
    size = vbuf.shape[3]

    levels = pairs.bit_length() - 1
    roles = sorted(range(pairs), key=lambda role: (role & 1 == 0, -role))

    def bit(level, side):
        return jnp.where(side == 0, 1 << level, 1 << (level + 1) % levels)

    def across(level, side):
        amount = bit(level, side)
        return amount * (1 - 2 * lax.rem(pair // amount, 2))

    def shard_of(role, other):
        side = 1 - core if other else core
        place = pair
        for level in range(levels):
            if role >> level & 1:
                place = place + across(level, side)
        return place * 2 + side

    def load(part, role, other):
        start = pl.multiple_of((shard_of(role, other) * PARTS + part) * size, size)
        slot = 2 * role + (0 if other else 1)
        return pltpu.make_async_copy(
            volt_ref.at[:, pl.ds(start, size)], vbuf.at[part, slot], load_sem.at[part, slot]
        )

    def begin(part, carry):
        for other in (True, False):
            for role in roles:
                load(part, role, other).start()
        return carry

    gains_copy = pltpu.make_async_copy(gains_hbm, gains_ref, side_sems.at[2])
    gains_copy.start()
    lax.fori_loop(0, PARTS, begin, 0)
    side = [
        pltpu.make_async_copy(chirp_hbm, chirp_ref, side_sems.at[0]),
        pltpu.make_async_copy(turns_hbm, turns_ref, side_sems.at[1]),
    ]
    for copy in side:
        copy.start()
    offset = offset_ref[0]
    gains_copy.wait()
    weight_table(gains_ref, table_ref, antennas, me)

    def pair_copy(part, role):
        return pltpu.make_async_remote_copy(
            src_ref=pair_send.at[part, role], dst_ref=pair_recv.at[part, role],
            send_sem=pair_sems.at[0, part, role], recv_sem=pair_sems.at[1, part, role],
            device_id={"tm": pair * 2 + (1 - core)}, device_id_type=MESH,
        )

    def level_of(role):
        return (role & -role).bit_length() - 1

    def chip_copy(part, role):
        slot = role - 1
        return pltpu.make_async_remote_copy(
            src_ref=chip_send.at[part, slot], dst_ref=chip_recv.at[part, slot],
            send_sem=chip_sems.at[0, part, slot], recv_sem=chip_sems.at[1, part, slot],
            device_id={"tm": (pair + across(level_of(role), core)) * 2 + core},
            device_id_type=MESH,
        )

    def halo_copy(part):
        return pltpu.make_async_remote_copy(
            src_ref=halo_send.at[part], dst_ref=halo_ref.at[part],
            send_sem=halo_sems.at[0, part], recv_sem=halo_sems.at[1, part],
            device_id={"tm": lax.rem(me + 1, count)}, device_id_type=MESH,
        )

    def head_copy():
        return pltpu.make_async_remote_copy(
            src_ref=halo_send.at[0, :, 0:HALO_ROWS], dst_ref=head_ref,
            send_sem=head_sems.at[0], recv_sem=head_sems.at[1],
            device_id={"tm": lax.rem(me + count - 1, count)}, device_id_type=MESH,
        )

    def pass_on(part, level):
        for role in roles:
            if role & ((2 << level) - 1) == 0:
                source = role + (1 << level)
                chip_copy(part, source).wait_recv()
                total = own_ref[part, role // 2] + chip_recv[part, source - 1].astype(jnp.float32)
                if role and level_of(role) == level + 1:
                    chip_send[part, role - 1] = total.astype(jnp.bfloat16)
                    chip_copy(part, role).start()
                else:
                    own_ref[part, role // 2] = total
                    if role == 0 and level == levels - 1:
                        halo_send[part] = total.astype(jnp.bfloat16)

    def finish(part):
        pass_on(part, levels - 1)

        @pl.when(me < count - 1)
        def _():
            halo_copy(part).start()

    def chirp_block(at):
        stride = ROWS // LANES
        for half in range(COLS // LANES):
            columns = chirp_ref[
                pl.ds(at + half * LANES * stride, LANES, stride=stride), :
            ]
            phase = jnp.transpose(columns, (1, 0))
            for out, value in enumerate(response(phase, at * LANES, half * LANES, offset)):
                block_ref[...] = value * (1.0 / NFFT)
                for parity in range(2):
                    rows = pl.ds(pl.multiple_of(at * (LANES // 2), LANES // 2), LANES // 2)
                    response_ref[out, parity, rows, half * LANES : (half + 1) * LANES] = (
                        block_ref[pl.ds(parity, LANES // 2, stride=2), :]
                    )

    def combine(part, first=None):
        rows = slice(part * PART_ROWS, (part + 1) * PART_ROWS)
        before = [halo_ref[part, out].astype(jnp.float32) for out in range(2)]
        if first is not None:
            before = [
                jnp.concatenate([head, value[HALO_ROWS:]], axis=0)
                for head, value in zip(first, before)
            ]
        after = [own_ref[part, 0, 0], own_ref[part, 0, 1]]
        real, imag = (before[0] - after[0], before[1] - after[1])
        cosine, sine = [
            jnp.concatenate([turns_ref[out, rows]] * (COLS // LANES), axis=1) for out in range(2)
        ]
        both = (
            (before[0] + after[0], before[1] + after[1]),
            (real * cosine - imag * sine, real * sine + imag * cosine),
        )
        for kind, values in enumerate(both):
            for out, value in enumerate(values):
                data_ref[kind, out, 0, rows], data_ref[kind, out, 1, rows] = split(value)

    def run(part, carry):
        for role in roles:
            load(part, role, True).wait()

            def put(out, at, rows, value, role=role):
                pair_send[part, role, out, at : at + rows] = value

            part_beam(table_ref, vbuf.at[part, 2 * role], antennas, put)
            if role == roles[0]:

                @pl.when(part == 0)
                def _():
                    pl.semaphore_wait(barrier, count - 1)

            pair_copy(part, role).start()
        for role in roles:
            load(part, role, False).wait()
            pair_copy(part, role).wait_recv()

            def put(out, at, rows, value, role=role):
                value = value + pair_recv[part, role, out, at : at + rows]
                if role % 2:
                    chip_send[part, role - 1, out, at : at + rows] = value.astype(jnp.bfloat16)
                else:
                    own_ref[part, role // 2, out, at : at + rows] = value

            part_beam(table_ref, vbuf.at[part, 2 * role + 1], antennas, put)
            if role % 2:
                chip_copy(part, role).start()
        return carry

    lax.fori_loop(0, PARTS, run, 0)
    for copy in side:
        copy.wait()

    def settle(part, carry):
        for level in range(levels - 1):
            pass_on(part, level)

        @pl.when(part < ROWS // LANES)
        def _():
            chirp_block(part)

        @pl.when(part > 0)
        def _():
            finish(part - 1)

            @pl.when((part == 1) & (me > 0))
            def _():
                head_copy().start()

        return carry

    lax.fori_loop(0, PARTS, settle, 0)
    finish(PARTS - 1)

    @pl.when(me == 0)
    def _():
        halo_ref[...] = jnp.zeros((PARTS, 2, PART_ROWS, COLS), jnp.bfloat16)

    @pl.when(me == count - 1)
    def _():
        head_ref[...] = jnp.zeros((2, HALO_ROWS, COLS), jnp.bfloat16)

    for part in range(PARTS):

        @pl.when(me > 0)
        def _():
            halo_copy(part).wait_recv()

        first = None
        if part == 0:

            @pl.when(me < count - 1)
            def _():
                head_copy().wait_recv()

            spot = lax.broadcasted_iota(jnp.int32, (HALO_ROWS, COLS), 0) * COLS
            spot = spot + lax.broadcasted_iota(jnp.int32, (HALO_ROWS, COLS), 1)
            first = [
                jnp.where(
                    spot < offset,
                    head_ref[out].astype(jnp.float32),
                    halo_ref[0, out, 0:HALO_ROWS].astype(jnp.float32),
                )
                for out in range(2)
            ]
        combine(part, first)

    @pl.when(me > 0)
    def _():
        head_copy().wait_send()

    @pl.when(me < count - 1)
    def _():
        for part in range(PARTS):
            halo_copy(part).wait_send()

    def drain(part, carry):
        for role in roles:
            pair_copy(part, role).wait_send()
            if role:
                chip_copy(part, role).wait_send()
        return carry

    lax.fori_loop(0, PARTS, drain, 0)


def beam(volts, gains, offset, chirp, shards):
    pairs = shards // 2
    size = volts.shape[1] // shards // PARTS
    antennas = size * LANES // (PART_ROWS * COLS)
    half = DEPTH // antennas // 2
    block = (2, PART_ROWS, COLS)
    vmem = pl.BlockSpec(memory_space=pltpu.VMEM)
    hbm = pl.BlockSpec(memory_space=pltpu.HBM)
    keep = functools.partial(pltpu.with_memory_space_constraint, memory_space=pltpu.HBM)
    return pl.pallas_call(
        functools.partial(beam_kernel, antennas, pairs),
        out_shape=(
            jax.ShapeDtypeStruct((2, 2, 2, HALF_ROWS, COLS), jnp.bfloat16),
            jax.ShapeDtypeStruct((2, 2, HALF_ROWS, COLS), jnp.float32),
        ),
        in_specs=[hbm, hbm, pl.BlockSpec(memory_space=pltpu.SMEM), hbm, hbm],
        out_specs=(vmem, vmem),
        scratch_shapes=[
            pltpu.VMEM((2, 8 * half, DEPTH), jnp.bfloat16),
            pltpu.VMEM((PARTS, shards, 2, size, LANES), jnp.bfloat16),
            pltpu.VMEM((PARTS, pairs) + block, jnp.float32),
            pltpu.VMEM((PARTS, pairs) + block, jnp.float32),
            pltpu.VMEM((PARTS, pairs - 1) + block, jnp.bfloat16),
            pltpu.VMEM((PARTS, pairs - 1) + block, jnp.bfloat16),
            pltpu.VMEM((PARTS, pairs // 2) + block, jnp.float32),
            pltpu.VMEM((PARTS,) + block, jnp.bfloat16),
            pltpu.VMEM((PARTS,) + block, jnp.bfloat16),
            pltpu.VMEM((2, HALO_ROWS, COLS), jnp.bfloat16),
            pltpu.VMEM(gains.shape, jnp.float32),
            pltpu.VMEM((NFFT // LANES, LANES), jnp.float32),
            pltpu.VMEM((2, HALF_ROWS, LANES), jnp.float32),
            pltpu.VMEM((LANES, LANES), jnp.float32),
            pltpu.SemaphoreType.DMA((PARTS, shards)),
            pltpu.SemaphoreType.DMA((2, PARTS, pairs)),
            pltpu.SemaphoreType.DMA((2, PARTS, pairs - 1)),
            pltpu.SemaphoreType.DMA((2, PARTS)),
            pltpu.SemaphoreType.DMA((2,)),
            pltpu.SemaphoreType.DMA((3,)),
        ],
        compiler_params=pltpu.CompilerParams(
            vmem_limit_bytes=44 << 20, collective_id=0, has_side_effects=True
        ),
        cost_estimate=pl.CostEstimate(
            flops=3 * 10**9, bytes_accessed=18 << 20, transcendentals=0
        ),
        name="beam",
    )(keep(volts), keep(gains), offset, keep(chirp), keep(jnp.asarray(half_turns())))


def fold_kernel(
    chans, shards, data_ref, response_ref, flags_ref, bins_ref, dft_ref, twist_ref, turns_ref,
    dedispersed_ref, small_ref, weighted_ref, high_ref, low_ref, send_ref, recv_ref,
    sems,
):
    everyone = chans * shards
    here = lax.axis_index("chan") * shards + lax.axis_index("tm")
    barrier = pltpu.get_barrier_semaphore()

    def target(index):
        return {"chan": index // shards, "tm": lax.rem(index, shards)}

    def greet(step, carry):
        pl.semaphore_signal(
            barrier, inc=1, device_id=target(lax.rem(here + step, everyone)), device_id_type=MESH
        )
        return carry

    lax.fori_loop(1, everyone, greet, 0)
    def table(start, count=1):
        rows = slice(start * COLS, (start + count) * COLS)
        return (dft_ref[0, rows], dft_ref[1, rows])

    minus_table, real_table, imag_table = (table(0), table(1), table(2))
    forward, cross = (table(1, 2), table(0, 2))
    pairs = []
    for kind in range(2):
        given = [(data_ref[kind, out, 0], data_ref[kind, out, 1]) for out in range(2)]
        both = product((forward, given[0]), (cross, given[1]))
        pairs.append((both[:HALF_ROWS], both[HALF_ROWS:]))
    for kind in range(2):
        real, imag = pairs[kind]
        cosine, sine = (twist_ref[0, kind], twist_ref[1, kind])
        pairs[kind] = (split(real * cosine - imag * sine), split(real * sine + imag * cosine))
    for kind in range(2):
        real, imag = pairs[kind]
        pairs[kind] = (
            product((real, real_table), (imag, minus_table)),
            product((real, imag_table), (imag, real_table)),
        )
    for kind in range(2):
        real, imag = pairs[kind]
        turn, tilt = (response_ref[0, kind], response_ref[1, kind])
        pairs[kind] = (split(real * turn - imag * tilt), split(real * tilt + imag * turn))
    for kind in range(2):
        real, imag = pairs[kind]
        pairs[kind] = (
            product((real, real_table), (imag, imag_table)),
            product((real, minus_table), (imag, real_table)),
        )
    for kind in range(2):
        real, imag = pairs[kind]
        cosine, sine = (twist_ref[0, kind], twist_ref[1, kind])
        pairs[kind] = (split(real * cosine + imag * sine), split(imag * cosine - real * sine))
    for kind in range(2):
        real, imag = pairs[kind]
        both = product((cross, real), (forward, imag))
        pairs[kind] = (both[HALF_ROWS:], both[:HALF_ROWS])

    flag = flags_ref[...]
    if WINDOWS < LANES:
        flag = jnp.concatenate([flag, jnp.zeros((1, LANES - WINDOWS), jnp.int32)], axis=1)
    keep_row = (1 - flag).astype(jnp.float32)
    shape = (BLOCK_ROWS, LANES)
    row_index = lax.broadcasted_iota(jnp.int32, shape, 0)
    lane_index = lax.broadcasted_iota(jnp.int32, shape, 1)

    def window_sum(values):
        total = jnp.broadcast_to(jnp.sum(values, axis=1, keepdims=True), shape)
        reach = 1
        while reach < WIN_ROWS:
            up, down = (pltpu.roll(total, BLOCK_ROWS - reach, 0), pltpu.roll(total, reach, 0))
            total = total + jnp.where(row_index % (2 * reach) < reach, up, down)
            reach *= 2
        return total

    per_line = COLS // LANES
    weight_row = jnp.zeros((1, LANES), jnp.float32)
    for start in range(0, HALF_ROWS, BLOCK_ROWS):
        rows = slice(start, start + BLOCK_ROWS)
        cosine, sine = [
            jnp.concatenate([turns_ref[out, rows]] * (COLS // LANES), axis=1) for out in range(2)
        ]
        (real, imag), (odd_real, odd_imag) = [[value[rows] for value in pair] for pair in pairs]
        real = real - (odd_real * cosine + odd_imag * sine)
        imag = imag - (odd_imag * cosine - odd_real * sine)
        dedispersed_ref[0, rows] = real.astype(jnp.bfloat16)
        dedispersed_ref[1, rows] = imag.astype(jnp.bfloat16)
        power = real * real + imag * imag
        first_sum, second_sum = (window_sum(power), window_sum(power * power))
        kurtosis = (
            (SKW + 1.0)
            / (SKW - 1.0)
            * (SKW * second_sum / (first_sum * first_sum + EPSILON) - 1.0)
        )
        scaled = (kurtosis - 1.0) / SK_WIDTH
        window = (row_index + start) // WIN_ROWS
        keep = jnp.where(lane_index == window, jnp.broadcast_to(keep_row, shape), 0.0)
        keep = jnp.sum(keep, axis=1, keepdims=True)
        sk_weight = keep / (1.0 + scaled * scaled)
        chosen = (row_index + start) == lane_index * WIN_ROWS
        weight_row = weight_row + jnp.sum(
            jnp.where(chosen, sk_weight, 0.0), axis=0, keepdims=True
        )
        for at in range(COLS // LANES):
            lanes = slice(at * LANES, (at + 1) * LANES)
            value = (sk_weight * power[:, lanes]).astype(jnp.bfloat16)
            places = pl.ds(start * per_line + at, BLOCK_ROWS, stride=per_line)
            weighted_ref[places, :] = value.astype(jnp.float32)

    bins = bins_ref[...]
    high_ref[...] = (bins // LOW_BINS).astype(jnp.float32)
    low_ref[...] = (bins % LOW_BINS).astype(jnp.float32)
    high_index = lax.broadcasted_iota(jnp.int32, (HIGH_BINS, LANES), 0)
    high_index = high_index.astype(jnp.float32).astype(jnp.bfloat16)
    low_index = lax.broadcasted_iota(jnp.int32, (LOW_BINS, LANES), 0)
    low_index = low_index.astype(jnp.float32).astype(jnp.bfloat16)
    minus, zero = (jnp.bfloat16(-1.0), jnp.bfloat16(0.0))

    def step(at, total):
        start = at * STEP_LINES
        left, right = ([], [])

        def spread(block, line, count):
            return jnp.broadcast_to(block[line : line + 1], (count, LANES)).astype(jnp.bfloat16)

        lines_here = pl.ds(start, STEP_LINES)
        highs, lows, values = (high_ref[lines_here], low_ref[lines_here], weighted_ref[lines_here])
        for line in range(STEP_LINES):
            left.append(jnp.where(high_index == spread(highs, line, HIGH_BINS), minus, zero))
            value = spread(values, line, LOW_BINS)
            right.append(jnp.where(low_index == spread(lows, line, LOW_BINS), value, zero))
        return total - lax.dot_general(
            jnp.concatenate(left, axis=1),
            jnp.concatenate(right, axis=1),
            ((((1,), (1,))), ((), ())),
            preferred_element_type=jnp.float32,
        )

    totals = [jnp.zeros((HIGH_BINS, LOW_BINS), jnp.float32)] * 2
    for at in range(HALF_ROWS * per_line // STEP_LINES):
        totals[at % 2] = step(at, totals[at % 2])
    total = totals[0] + totals[1]
    per_row = LANES // LOW_BINS
    total = jnp.concatenate([total, jnp.zeros((HIGH_BINS, LANES - LOW_BINS), jnp.float32)], axis=1)
    place = lax.broadcasted_iota(jnp.int32, (HIGH_BINS, LANES), 0) % per_row
    moved = jnp.where(place == 0, total, 0.0)
    for at in range(1, per_row):
        moved = moved + jnp.where(place == at, pltpu.roll(total, at * LOW_BINS, 1), 0.0)
    lines = BINS // LANES // shards
    for line in range(BINS // LANES):
        send_ref[line // lines, line % lines : line % lines + 1] = jnp.sum(
            moved[line * per_row : (line + 1) * per_row], axis=0, keepdims=True
        )
    pl.semaphore_wait(barrier, everyone - 1)

    def outgoing(index):
        return pltpu.make_async_remote_copy(
            src_ref=send_ref.at[lax.rem(index, shards)], dst_ref=recv_ref.at[here],
            send_sem=sems.at[0, index], recv_sem=sems.at[1, here],
            device_id=target(index), device_id_type=MESH,
        )

    def incoming(index):
        return pltpu.make_async_remote_copy(
            src_ref=send_ref.at[lax.rem(index, shards)], dst_ref=recv_ref.at[index],
            send_sem=sems.at[0, index], recv_sem=sems.at[1, index],
            device_id=target(index), device_id_type=MESH,
        )

    def begin(step, carry):
        outgoing(lax.rem(here + step, everyone)).start()
        return carry

    def arrive(step, carry):
        incoming(lax.rem(here + everyone - step, everyone)).wait_recv()
        return carry

    def leave(step, carry):
        outgoing(lax.rem(here + step, everyone)).wait_send()
        return carry

    lax.fori_loop(1, everyone, begin, 0)
    recv_ref[here] = send_ref[lax.axis_index("tm")]
    lax.fori_loop(1, everyone, arrive, 0)
    scale = BINS / (HALF_ROWS * COLS * shards)
    band = None
    mine = lax.axis_index("chan")
    for chan in range(chans):
        line = recv_ref[chan * shards]
        for at in range(1, shards):
            line = line + recv_ref[chan * shards + at]
        line = line * scale
        own = jnp.where(mine == chan, line, 0.0)
        band, profile = (line, own) if band is None else (band + line, profile + own)
    small_ref[0:lines] = profile
    small_ref[lines : 2 * lines] = band
    small_ref[2 * lines : 2 * lines + 1] = weight_row
    lax.fori_loop(1, everyone, leave, 0)


def fold(data, reply, flags, bins, chans, shards):
    vmem = pl.BlockSpec(memory_space=pltpu.VMEM)
    tables = (dft_table(), twiddle(), half_turns())
    lines = BINS // LANES // shards
    return pl.pallas_call(
        functools.partial(fold_kernel, chans, shards),
        out_shape=(
            jax.ShapeDtypeStruct((2, HALF_ROWS, COLS), jnp.bfloat16),
            jax.ShapeDtypeStruct((2 * lines + 1, LANES), jnp.float32),
        ),
        in_specs=[vmem] * 7,
        out_specs=(vmem,) * 2,
        scratch_shapes=[
            pltpu.VMEM((HALF_ROWS * COLS // LANES, LANES), jnp.float32),
            pltpu.VMEM((HALF_ROWS * COLS // LANES, LANES), jnp.float32),
            pltpu.VMEM((HALF_ROWS * COLS // LANES, LANES), jnp.float32),
            pltpu.VMEM((shards, lines, LANES), jnp.float32),
            pltpu.VMEM((chans * shards, lines, LANES), jnp.float32),
            pltpu.SemaphoreType.DMA((2, chans * shards)),
        ],
        compiler_params=pltpu.CompilerParams(
            vmem_limit_bytes=40 << 20, collective_id=1, has_side_effects=True
        ),
        cost_estimate=pl.CostEstimate(
            flops=6 * 10**9, bytes_accessed=6 << 20, transcendentals=0
        ),
        name="fold",
    )(data, reply, flags, bins, *[jnp.asarray(table) for table in tables])


def on_device(voltages, antenna_gains, chirp_phase, offsets, flags, sample_phase_bins):
    shards, chans = (lax.axis_size("tm"), lax.axis_size("chan"))
    antennas, channels, samples = voltages.shape[1:]
    assert channels == 1 and shards >= 4 and shards & (shards - 1) == 0
    volts = voltages.reshape(2, antennas, samples // LANES, LANES)
    volts = jnp.transpose(volts, (0, 2, 1, 3)).reshape(2, samples // LANES * antennas, LANES)
    gains = jnp.transpose(antenna_gains, (0, 2, 1))
    data, reply = beam(volts, gains, offsets, chirp_phase.reshape(-1, LANES), shards)
    bins = sample_phase_bins.reshape(-1, LANES)
    dedispersed, small = fold(data, reply, flags, bins, chans, shards)
    lines = BINS // LANES // shards
    return (
        dedispersed.reshape(2, 1, HALF_ROWS * COLS),
        small[2 * lines : 2 * lines + 1, :WINDOWS],
        small[:lines].reshape(1, BINS // shards),
        small[lines : 2 * lines].reshape(BINS // shards),
    )


def solution(mesh):
    placed = (
        P(None, "tm", "chan", None),
        P(None, None, "chan"),
        P("chan", None),
        P("chan"),
        P("chan", "tm"),
        P("tm"),
    )
    return jax.shard_map(
        on_device,
        mesh=mesh,
        in_specs=placed,
        out_specs=(P(None, "chan", "tm"), P("chan", "tm"), P("chan", "tm"), P("tm")),
        check_vma=False,
    )
```

```python
import functools
import math

import jax
import jax.numpy as jnp
import numpy as np
from jax import lax
from jax.experimental import pallas as pl
from jax.experimental.pallas import tpu as pltpu
from jax.sharding import PartitionSpec as P

NFFT = 131072
OFFSET_BOUND = 4096
SKW = 1024
BINS = 2048


SK_WIDTH = 0.05
EPSILON = 1e-06

COLS = 1 << (NFFT.bit_length() - 1) // 2
ROWS = NFFT // COLS
HALF_ROWS = ROWS // 2
HALO_ROWS = OFFSET_BOUND // COLS
WIN_ROWS = SKW // COLS
WINDOWS = HALF_ROWS // WIN_ROWS
LOW_BINS = 32
HIGH_BINS = BINS // LOW_BINS
BLOCK_ROWS = 128
STEP_LINES = 8
LANES = 128
DEPTH = 256
PARTS = 8
PAIR_LAG = 2
CHIP_LAG = 5
PART_ROWS = HALF_ROWS // PARTS
MESH = pl.DeviceIdType.MESH


def bf16_split(table):
    high = table.astype(jnp.bfloat16)
    low = (table - high.astype(np.float32)).astype(jnp.bfloat16)
    return np.stack([high, low])


def unit_roots(turns, period):
    angle = -2.0 * math.pi / period * (turns % period)
    return (np.cos(angle).astype(np.float32), np.sin(angle).astype(np.float32))


def dft_table():
    index = np.arange(COLS, dtype=np.int64)
    real, imag = unit_roots(index[:, None] * index[None, :], COLS)
    return bf16_split(np.concatenate([-imag, real, imag]))


def twiddle():
    index = np.arange(HALF_ROWS, dtype=np.int64)
    rows = np.stack([2 * index, 2 * index + 1])
    return np.stack(unit_roots(rows[:, :, None] * np.arange(COLS, dtype=np.int64), NFFT))


def half_turns():
    index = np.arange(HALF_ROWS, dtype=np.int64)
    return np.stack(unit_roots(np.repeat(index[:, None], LANES, axis=1), ROWS))


def split(value):
    high = value.astype(jnp.bfloat16)
    return high, (value - high.astype(jnp.float32)).astype(jnp.bfloat16)


def product(*pairs):
    left, right = ([], [])
    for a, b in pairs:
        left += [a[0], a[0], a[1]]
        right += [b[0], b[1], b[0]]
    return jnp.dot(
        jnp.concatenate(left, axis=1),
        jnp.concatenate(right, axis=0),
        preferred_element_type=jnp.float32,
    )


def cos_sin(angle):
    half = 0.5 * angle
    square = half * half
    sine = jnp.full_like(square, 1.0 / math.factorial(13))
    for power in (11, 9, 7, 5, 3, 1):
        sine = sine * square + (-1.0) ** (power // 2) / math.factorial(power)
    sine = sine * half
    cosine = jnp.full_like(square, 1.0 / math.factorial(12))
    for power in (10, 8, 6, 4, 2, 0):
        cosine = cosine * square + (-1.0) ** (power // 2) / math.factorial(power)
    return 1.0 - 2.0 * sine * sine, 2.0 * sine * cosine


def response(phase, first, first_column, offset):
    index = first + lax.broadcasted_iota(jnp.int32, phase.shape, 0)
    column = first_column + lax.broadcasted_iota(jnp.int32, phase.shape, 1)
    index = index + ROWS * column
    turns = (index * offset) & (NFFT - 1)
    turns = jnp.where(turns >= NFFT // 2, turns - NFFT, turns)
    phase = phase + turns.astype(jnp.float32) * (2.0 * math.pi / NFFT)
    phase = jnp.where(phase > math.pi, phase - 2.0 * math.pi, phase)
    phase = jnp.where(phase < -math.pi, phase + 2.0 * math.pi, phase)
    return cos_sin(phase)


def weight_table(gains_ref, table_ref, antennas, me):
    total = gains_ref.shape[2]
    lane = lax.broadcasted_iota(jnp.int32, (8, LANES), 1)
    wide = []
    for part in range(2):
        row = gains_ref[part]
        if total < LANES:
            row = jnp.concatenate([row, jnp.zeros((1, LANES - total), jnp.float32)], axis=1)
        row = jnp.broadcast_to(row, (8, LANES))
        row = pltpu.roll(row, lax.rem(LANES - me * antennas, LANES), 1)
        row = jnp.where(lane < antennas, row, 0.0)
        width = antennas
        while width < LANES:
            row = row + pltpu.roll(row, width, 1)
            width *= 2
        wide.append(jnp.concatenate([row] * (DEPTH // LANES), axis=1)[:1])
    real, imag = wide
    half = DEPTH // antennas // 2
    shape = (half, DEPTH)
    tile = lax.broadcasted_iota(jnp.int32, shape, 1) // antennas
    index = lax.broadcasted_iota(jnp.int32, shape, 0)
    for source, pair in enumerate(((real, imag), (-imag, real))):
        for out, values in enumerate(pair):
            for parity in range(2):
                dense = jnp.where(tile == 2 * index + parity, values, 0.0)
                high, low = split(dense)
                at = (2 * out + parity) * half
                table_ref[source, at : at + half] = high
                table_ref[source, 4 * half + at : 4 * half + at + half] = low


def part_beam(table_ref, volt_ref, antennas, put):
    half = DEPTH // antennas // 2
    groups = volt_ref.shape[1] // DEPTH
    joined = 2 if groups % 2 == 0 else 1
    for at in range(groups // joined):
        total = None
        for source in range(2):
            lanes = [
                volt_ref[source, (joined * at + b) * DEPTH : (joined * at + b + 1) * DEPTH]
                for b in range(joined)
            ]
            right = lanes[0] if joined == 1 else jnp.concatenate(lanes, axis=1)
            term = jnp.dot(table_ref[source], right, preferred_element_type=jnp.float32)
            total = term if total is None else total + term
        total = total[: 4 * half] + total[4 * half :]
        for b in range(joined):
            block = total[:, b * LANES : (b + 1) * LANES]
            for out in range(2):
                even = block[2 * out * half : (2 * out + 1) * half]
                odd = block[(2 * out + 1) * half : (2 * out + 2) * half]
                put(out, (joined * at + b) * half, half, jnp.concatenate([even, odd], axis=1))


def beam_kernel(
    antennas, pairs, volt_ref, gains_hbm, offset_ref, chirp_hbm, turns_hbm, data_ref, response_ref,
    table_ref, vbuf, pair_send, pair_recv, chip_send, chip_recv, own_ref, halo_send, halo_ref,
    head_ref, gains_ref, chirp_ref, turns_ref, block_ref, load_sem, pair_sems, chip_sems, halo_sems,
    head_sems, side_sems,
):
    count = 2 * pairs
    me = lax.axis_index("tm")
    pair, core = (me // 2, lax.rem(me, 2))
    barrier = pltpu.get_barrier_semaphore()
    for step in range(1, count):
        pl.semaphore_signal(
            barrier, inc=1, device_id={"tm": lax.rem(me + step, count)}, device_id_type=MESH
        )
    size = vbuf.shape[3]

    levels = pairs.bit_length() - 1
    roles = sorted(range(pairs), key=lambda role: (role & 1 == 0, -role))

    def bit(level, side):
        return jnp.where(side == 0, 1 << level, 1 << (level + 1) % levels)

    def across(level, side):
        amount = bit(level, side)
        return amount * (1 - 2 * lax.rem(pair // amount, 2))

    def shard_of(role, other):
        side = 1 - core if other else core
        place = pair
        for level in range(levels):
            if role >> level & 1:
                place = place + across(level, side)
        return place * 2 + side

    def load(part, role, other):
        start = pl.multiple_of((shard_of(role, other) * PARTS + part) * size, size)
        slot = 2 * role + (0 if other else 1)
        return pltpu.make_async_copy(
            volt_ref.at[:, pl.ds(start, size)], vbuf.at[part, slot], load_sem.at[part, slot]
        )

    def begin(step, carry):
        @pl.when(step < PARTS)
        def _():
            for role in roles:
                load(step, role, True).start()

        @pl.when(step >= PAIR_LAG)
        def _():
            for role in roles:
                load(step - PAIR_LAG, role, False).start()

        return carry

    gains_copy = pltpu.make_async_copy(gains_hbm, gains_ref, side_sems.at[2])
    gains_copy.start()
    lax.fori_loop(0, PARTS + PAIR_LAG, begin, 0)
    side = [
        pltpu.make_async_copy(chirp_hbm, chirp_ref, side_sems.at[0]),
        pltpu.make_async_copy(turns_hbm, turns_ref, side_sems.at[1]),
    ]
    for copy in side:
        copy.start()
    offset = offset_ref[0]
    gains_copy.wait()
    weight_table(gains_ref, table_ref, antennas, me)

    def pair_copy(part):
        return pltpu.make_async_remote_copy(
            src_ref=pair_send.at[part], dst_ref=pair_recv.at[part],
            send_sem=pair_sems.at[0, part], recv_sem=pair_sems.at[1, part],
            device_id={"tm": pair * 2 + (1 - core)}, device_id_type=MESH,
        )

    def level_of(role):
        return (role & -role).bit_length() - 1

    def first_slot(level):
        return pairs - (pairs >> level)

    def slot_of(role):
        level = level_of(role)
        return first_slot(level) + (role >> (level + 1))

    def chip_copy(part, level):
        slots = slice(first_slot(level), first_slot(level + 1))
        return pltpu.make_async_remote_copy(
            src_ref=chip_send.at[part, slots], dst_ref=chip_recv.at[part, slots],
            send_sem=chip_sems.at[0, part, level], recv_sem=chip_sems.at[1, part, level],
            device_id={"tm": (pair + across(level, core)) * 2 + core}, device_id_type=MESH,
        )

    def halo_copy(part):
        return pltpu.make_async_remote_copy(
            src_ref=halo_send.at[part], dst_ref=halo_ref.at[part],
            send_sem=halo_sems.at[0, part], recv_sem=halo_sems.at[1, part],
            device_id={"tm": lax.rem(me + 1, count)}, device_id_type=MESH,
        )

    def head_copy():
        return pltpu.make_async_remote_copy(
            src_ref=halo_send.at[0, :, 0:HALO_ROWS], dst_ref=head_ref,
            send_sem=head_sems.at[0], recv_sem=head_sems.at[1],
            device_id={"tm": lax.rem(me + count - 1, count)}, device_id_type=MESH,
        )

    def pass_on(part, level):
        chip_copy(part, level).wait_recv()
        for role in roles:
            if role & ((2 << level) - 1) == 0:
                arrived = chip_recv[part, slot_of(role + (1 << level))].astype(jnp.float32)
                total = own_ref[part, role // 2] + arrived
                if role and level_of(role) == level + 1:
                    chip_send[part, slot_of(role)] = total.astype(jnp.bfloat16)
                else:
                    own_ref[part, role // 2] = total
                    if role == 0 and level == levels - 1:
                        halo_send[part] = total.astype(jnp.bfloat16)
        if level < levels - 1:
            chip_copy(part, level + 1).start()

    def finish(part):
        pass_on(part, levels - 1)

        @pl.when(me < count - 1)
        def _():
            halo_copy(part).start()

    def chirp_block(at):
        stride = ROWS // LANES
        for half in range(COLS // LANES):
            columns = chirp_ref[
                pl.ds(at + half * LANES * stride, LANES, stride=stride), :
            ]
            phase = jnp.transpose(columns, (1, 0))
            for out, value in enumerate(response(phase, at * LANES, half * LANES, offset)):
                block_ref[...] = value * (1.0 / NFFT)
                for parity in range(2):
                    rows = pl.ds(pl.multiple_of(at * (LANES // 2), LANES // 2), LANES // 2)
                    response_ref[out, parity, rows, half * LANES : (half + 1) * LANES] = (
                        block_ref[pl.ds(parity, LANES // 2, stride=2), :]
                    )

    def combine(part, first=None):
        rows = slice(part * PART_ROWS, (part + 1) * PART_ROWS)
        before = [halo_ref[part, out].astype(jnp.float32) for out in range(2)]
        if first is not None:
            before = [
                jnp.concatenate([head, value[HALO_ROWS:]], axis=0)
                for head, value in zip(first, before)
            ]
        after = [own_ref[part, 0, 0], own_ref[part, 0, 1]]
        real, imag = (before[0] - after[0], before[1] - after[1])
        cosine, sine = [
            jnp.concatenate([turns_ref[out, rows]] * (COLS // LANES), axis=1) for out in range(2)
        ]
        both = (
            (before[0] + after[0], before[1] + after[1]),
            (real * cosine - imag * sine, real * sine + imag * cosine),
        )
        for kind, values in enumerate(both):
            for out, value in enumerate(values):
                data_ref[kind, out, 0, rows], data_ref[kind, out, 1, rows] = split(value)

    def give(part):
        for role in roles:
            load(part, role, True).wait()
        for role in roles:

            def put(out, at, rows, value, role=role):
                pair_send[part, role, out, at : at + rows] = value

            part_beam(table_ref, vbuf.at[part, 2 * role], antennas, put)

        @pl.when(part == 0)
        def _():
            pl.semaphore_wait(barrier, count - 1)

        pair_copy(part).start()

    def take(part):
        for role in roles:
            load(part, role, False).wait()
        pair_copy(part).wait_recv()
        for role in roles:

            def put(out, at, rows, value, role=role):
                value = value + pair_recv[part, role, out, at : at + rows]
                if role % 2:
                    chip_send[part, slot_of(role), out, at : at + rows] = value.astype(jnp.bfloat16)
                else:
                    own_ref[part, role // 2, out, at : at + rows] = value

            part_beam(table_ref, vbuf.at[part, 2 * role + 1], antennas, put)
        chip_copy(part, 0).start()

    def run(step, carry):
        @pl.when(step < PARTS)
        def _():
            give(step)

        @pl.when(step >= PAIR_LAG)
        def _():
            take(step - PAIR_LAG)

        return carry

    lax.fori_loop(0, PARTS + PAIR_LAG, run, 0)
    for copy in side:
        copy.wait()

    def settle(step, carry):
        @pl.when(step < PARTS)
        def _():
            for level in range(levels - 1):
                pass_on(step, level)

        @pl.when(step < ROWS // LANES)
        def _():
            chirp_block(step)

        @pl.when(step >= CHIP_LAG)
        def _():
            finish(step - CHIP_LAG)

            @pl.when((step == CHIP_LAG) & (me > 0))
            def _():
                head_copy().start()

        return carry

    lax.fori_loop(0, PARTS + CHIP_LAG, settle, 0)

    @pl.when(me == 0)
    def _():
        halo_ref[...] = jnp.zeros((PARTS, 2, PART_ROWS, COLS), jnp.bfloat16)

    @pl.when(me == count - 1)
    def _():
        head_ref[...] = jnp.zeros((2, HALO_ROWS, COLS), jnp.bfloat16)

    for part in range(PARTS):

        @pl.when(me > 0)
        def _():
            halo_copy(part).wait_recv()

        first = None
        if part == 0:

            @pl.when(me < count - 1)
            def _():
                head_copy().wait_recv()

            spot = lax.broadcasted_iota(jnp.int32, (HALO_ROWS, COLS), 0) * COLS
            spot = spot + lax.broadcasted_iota(jnp.int32, (HALO_ROWS, COLS), 1)
            first = [
                jnp.where(
                    spot < offset,
                    head_ref[out].astype(jnp.float32),
                    halo_ref[0, out, 0:HALO_ROWS].astype(jnp.float32),
                )
                for out in range(2)
            ]
        combine(part, first)

    @pl.when(me > 0)
    def _():
        head_copy().wait_send()

    @pl.when(me < count - 1)
    def _():
        for part in range(PARTS):
            halo_copy(part).wait_send()

    def drain(part, carry):
        pair_copy(part).wait_send()
        for level in range(levels):
            chip_copy(part, level).wait_send()
        return carry

    lax.fori_loop(0, PARTS, drain, 0)


def beam(volts, gains, offset, chirp, shards):
    pairs = shards // 2
    size = volts.shape[1] // shards // PARTS
    antennas = size * LANES // (PART_ROWS * COLS)
    half = DEPTH // antennas // 2
    block = (2, PART_ROWS, COLS)
    vmem = pl.BlockSpec(memory_space=pltpu.VMEM)
    hbm = pl.BlockSpec(memory_space=pltpu.HBM)
    keep = functools.partial(pltpu.with_memory_space_constraint, memory_space=pltpu.HBM)
    return pl.pallas_call(
        functools.partial(beam_kernel, antennas, pairs),
        out_shape=(
            jax.ShapeDtypeStruct((2, 2, 2, HALF_ROWS, COLS), jnp.bfloat16),
            jax.ShapeDtypeStruct((2, 2, HALF_ROWS, COLS), jnp.float32),
        ),
        in_specs=[hbm, hbm, pl.BlockSpec(memory_space=pltpu.SMEM), hbm, hbm],
        out_specs=(vmem, vmem),
        scratch_shapes=[
            pltpu.VMEM((2, 8 * half, DEPTH), jnp.bfloat16),
            pltpu.VMEM((PARTS, shards, 2, size, LANES), jnp.bfloat16),
            pltpu.VMEM((PARTS, pairs) + block, jnp.float32),
            pltpu.VMEM((PARTS, pairs) + block, jnp.float32),
            pltpu.VMEM((PARTS, pairs - 1) + block, jnp.bfloat16),
            pltpu.VMEM((PARTS, pairs - 1) + block, jnp.bfloat16),
            pltpu.VMEM((PARTS, pairs // 2) + block, jnp.float32),
            pltpu.VMEM((PARTS,) + block, jnp.bfloat16),
            pltpu.VMEM((PARTS,) + block, jnp.bfloat16),
            pltpu.VMEM((2, HALO_ROWS, COLS), jnp.bfloat16),
            pltpu.VMEM(gains.shape, jnp.float32),
            pltpu.VMEM((NFFT // LANES, LANES), jnp.float32),
            pltpu.VMEM((2, HALF_ROWS, LANES), jnp.float32),
            pltpu.VMEM((LANES, LANES), jnp.float32),
            pltpu.SemaphoreType.DMA((PARTS, shards)),
            pltpu.SemaphoreType.DMA((2, PARTS)),
            pltpu.SemaphoreType.DMA((2, PARTS, pairs.bit_length() - 1)),
            pltpu.SemaphoreType.DMA((2, PARTS)),
            pltpu.SemaphoreType.DMA((2,)),
            pltpu.SemaphoreType.DMA((3,)),
        ],
        compiler_params=pltpu.CompilerParams(
            vmem_limit_bytes=44 << 20, collective_id=0, has_side_effects=True
        ),
        cost_estimate=pl.CostEstimate(
            flops=3 * 10**9, bytes_accessed=18 << 20, transcendentals=0
        ),
        name="beam",
    )(keep(volts), keep(gains), offset, keep(chirp), keep(jnp.asarray(half_turns())))


def fold_kernel(
    chans, shards, data_ref, response_ref, flags_ref, bins_ref, dft_ref, twist_ref, turns_ref,
    dedispersed_ref, small_ref, weighted_ref, high_ref, low_ref, send_ref, recv_ref,
    sems,
):
    everyone = chans * shards
    here = lax.axis_index("chan") * shards + lax.axis_index("tm")
    barrier = pltpu.get_barrier_semaphore()

    def target(index):
        return {"chan": index // shards, "tm": lax.rem(index, shards)}

    def greet(step, carry):
        pl.semaphore_signal(
            barrier, inc=1, device_id=target(lax.rem(here + step, everyone)), device_id_type=MESH
        )
        return carry

    lax.fori_loop(1, everyone, greet, 0)
    def table(start, count=1):
        rows = slice(start * COLS, (start + count) * COLS)
        return (dft_ref[0, rows], dft_ref[1, rows])

    minus_table, real_table, imag_table = (table(0), table(1), table(2))
    forward, cross = (table(1, 2), table(0, 2))
    pairs = []
    for kind in range(2):
        given = [(data_ref[kind, out, 0], data_ref[kind, out, 1]) for out in range(2)]
        both = product((forward, given[0]), (cross, given[1]))
        pairs.append((both[:HALF_ROWS], both[HALF_ROWS:]))
    for kind in range(2):
        real, imag = pairs[kind]
        cosine, sine = (twist_ref[0, kind], twist_ref[1, kind])
        pairs[kind] = (split(real * cosine - imag * sine), split(real * sine + imag * cosine))
    for kind in range(2):
        real, imag = pairs[kind]
        pairs[kind] = (
            product((real, real_table), (imag, minus_table)),
            product((real, imag_table), (imag, real_table)),
        )
    for kind in range(2):
        real, imag = pairs[kind]
        turn, tilt = (response_ref[0, kind], response_ref[1, kind])
        pairs[kind] = (split(real * turn - imag * tilt), split(real * tilt + imag * turn))
    for kind in range(2):
        real, imag = pairs[kind]
        pairs[kind] = (
            product((real, real_table), (imag, imag_table)),
            product((real, minus_table), (imag, real_table)),
        )
    for kind in range(2):
        real, imag = pairs[kind]
        cosine, sine = (twist_ref[0, kind], twist_ref[1, kind])
        pairs[kind] = (split(real * cosine + imag * sine), split(imag * cosine - real * sine))
    for kind in range(2):
        real, imag = pairs[kind]
        both = product((cross, real), (forward, imag))
        pairs[kind] = (both[HALF_ROWS:], both[:HALF_ROWS])

    flag = flags_ref[...]
    if WINDOWS < LANES:
        flag = jnp.concatenate([flag, jnp.zeros((1, LANES - WINDOWS), jnp.int32)], axis=1)
    keep_row = (1 - flag).astype(jnp.float32)
    shape = (BLOCK_ROWS, LANES)
    row_index = lax.broadcasted_iota(jnp.int32, shape, 0)
    lane_index = lax.broadcasted_iota(jnp.int32, shape, 1)

    def window_sum(values):
        total = jnp.broadcast_to(jnp.sum(values, axis=1, keepdims=True), shape)
        reach = 1
        while reach < WIN_ROWS:
            up, down = (pltpu.roll(total, BLOCK_ROWS - reach, 0), pltpu.roll(total, reach, 0))
            total = total + jnp.where(row_index % (2 * reach) < reach, up, down)
            reach *= 2
        return total

    per_line = COLS // LANES
    weight_row = jnp.zeros((1, LANES), jnp.float32)
    for start in range(0, HALF_ROWS, BLOCK_ROWS):
        rows = slice(start, start + BLOCK_ROWS)
        cosine, sine = [
            jnp.concatenate([turns_ref[out, rows]] * (COLS // LANES), axis=1) for out in range(2)
        ]
        (real, imag), (odd_real, odd_imag) = [[value[rows] for value in pair] for pair in pairs]
        real = real - (odd_real * cosine + odd_imag * sine)
        imag = imag - (odd_imag * cosine - odd_real * sine)
        dedispersed_ref[0, rows] = real.astype(jnp.bfloat16)
        dedispersed_ref[1, rows] = imag.astype(jnp.bfloat16)
        power = real * real + imag * imag
        first_sum, second_sum = (window_sum(power), window_sum(power * power))
        kurtosis = (
            (SKW + 1.0)
            / (SKW - 1.0)
            * (SKW * second_sum / (first_sum * first_sum + EPSILON) - 1.0)
        )
        scaled = (kurtosis - 1.0) / SK_WIDTH
        window = (row_index + start) // WIN_ROWS
        keep = jnp.where(lane_index == window, jnp.broadcast_to(keep_row, shape), 0.0)
        keep = jnp.sum(keep, axis=1, keepdims=True)
        sk_weight = keep / (1.0 + scaled * scaled)
        chosen = (row_index + start) == lane_index * WIN_ROWS
        weight_row = weight_row + jnp.sum(
            jnp.where(chosen, sk_weight, 0.0), axis=0, keepdims=True
        )
        for at in range(COLS // LANES):
            lanes = slice(at * LANES, (at + 1) * LANES)
            value = (sk_weight * power[:, lanes]).astype(jnp.bfloat16)
            places = pl.ds(start * per_line + at, BLOCK_ROWS, stride=per_line)
            weighted_ref[places, :] = value.astype(jnp.float32)

    bins = bins_ref[...]
    high_ref[...] = (bins // LOW_BINS).astype(jnp.float32)
    low_ref[...] = (bins % LOW_BINS).astype(jnp.float32)
    high_index = lax.broadcasted_iota(jnp.int32, (HIGH_BINS, LANES), 0)
    high_index = high_index.astype(jnp.float32).astype(jnp.bfloat16)
    low_index = lax.broadcasted_iota(jnp.int32, (LOW_BINS, LANES), 0)
    low_index = low_index.astype(jnp.float32).astype(jnp.bfloat16)
    minus, zero = (jnp.bfloat16(-1.0), jnp.bfloat16(0.0))

    def step(at, total):
        start = at * STEP_LINES
        left, right = ([], [])

        def spread(block, line, count):
            return jnp.broadcast_to(block[line : line + 1], (count, LANES)).astype(jnp.bfloat16)

        lines_here = pl.ds(start, STEP_LINES)
        highs, lows, values = (high_ref[lines_here], low_ref[lines_here], weighted_ref[lines_here])
        for line in range(STEP_LINES):
            left.append(jnp.where(high_index == spread(highs, line, HIGH_BINS), minus, zero))
            value = spread(values, line, LOW_BINS)
            right.append(jnp.where(low_index == spread(lows, line, LOW_BINS), value, zero))
        return total - lax.dot_general(
            jnp.concatenate(left, axis=1),
            jnp.concatenate(right, axis=1),
            ((((1,), (1,))), ((), ())),
            preferred_element_type=jnp.float32,
        )

    totals = [jnp.zeros((HIGH_BINS, LOW_BINS), jnp.float32)] * 2
    for at in range(HALF_ROWS * per_line // STEP_LINES):
        totals[at % 2] = step(at, totals[at % 2])
    total = totals[0] + totals[1]
    per_row = LANES // LOW_BINS
    total = jnp.concatenate([total, jnp.zeros((HIGH_BINS, LANES - LOW_BINS), jnp.float32)], axis=1)
    place = lax.broadcasted_iota(jnp.int32, (HIGH_BINS, LANES), 0) % per_row
    moved = jnp.where(place == 0, total, 0.0)
    for at in range(1, per_row):
        moved = moved + jnp.where(place == at, pltpu.roll(total, at * LOW_BINS, 1), 0.0)
    lines = BINS // LANES // shards
    for line in range(BINS // LANES):
        send_ref[line // lines, line % lines : line % lines + 1] = jnp.sum(
            moved[line * per_row : (line + 1) * per_row], axis=0, keepdims=True
        )
    pl.semaphore_wait(barrier, everyone - 1)

    def outgoing(index):
        return pltpu.make_async_remote_copy(
            src_ref=send_ref.at[lax.rem(index, shards)], dst_ref=recv_ref.at[here],
            send_sem=sems.at[0, index], recv_sem=sems.at[1, here],
            device_id=target(index), device_id_type=MESH,
        )

    def incoming(index):
        return pltpu.make_async_remote_copy(
            src_ref=send_ref.at[lax.rem(index, shards)], dst_ref=recv_ref.at[index],
            send_sem=sems.at[0, index], recv_sem=sems.at[1, index],
            device_id=target(index), device_id_type=MESH,
        )

    def begin(step, carry):
        outgoing(lax.rem(here + step, everyone)).start()
        return carry

    def arrive(step, carry):
        incoming(lax.rem(here + everyone - step, everyone)).wait_recv()
        return carry

    def leave(step, carry):
        outgoing(lax.rem(here + step, everyone)).wait_send()
        return carry

    lax.fori_loop(1, everyone, begin, 0)
    recv_ref[here] = send_ref[lax.axis_index("tm")]
    lax.fori_loop(1, everyone, arrive, 0)
    scale = BINS / (HALF_ROWS * COLS * shards)
    band = None
    mine = lax.axis_index("chan")
    for chan in range(chans):
        line = recv_ref[chan * shards]
        for at in range(1, shards):
            line = line + recv_ref[chan * shards + at]
        line = line * scale
        own = jnp.where(mine == chan, line, 0.0)
        band, profile = (line, own) if band is None else (band + line, profile + own)
    small_ref[0:lines] = profile
    small_ref[lines : 2 * lines] = band
    small_ref[2 * lines : 2 * lines + 1] = weight_row
    lax.fori_loop(1, everyone, leave, 0)


def fold(data, reply, flags, bins, chans, shards):
    vmem = pl.BlockSpec(memory_space=pltpu.VMEM)
    tables = (dft_table(), twiddle(), half_turns())
    lines = BINS // LANES // shards
    return pl.pallas_call(
        functools.partial(fold_kernel, chans, shards),
        out_shape=(
            jax.ShapeDtypeStruct((2, HALF_ROWS, COLS), jnp.bfloat16),
            jax.ShapeDtypeStruct((2 * lines + 1, LANES), jnp.float32),
        ),
        in_specs=[vmem] * 7,
        out_specs=(vmem,) * 2,
        scratch_shapes=[
            pltpu.VMEM((HALF_ROWS * COLS // LANES, LANES), jnp.float32),
            pltpu.VMEM((HALF_ROWS * COLS // LANES, LANES), jnp.float32),
            pltpu.VMEM((HALF_ROWS * COLS // LANES, LANES), jnp.float32),
            pltpu.VMEM((shards, lines, LANES), jnp.float32),
            pltpu.VMEM((chans * shards, lines, LANES), jnp.float32),
            pltpu.SemaphoreType.DMA((2, chans * shards)),
        ],
        compiler_params=pltpu.CompilerParams(
            vmem_limit_bytes=40 << 20, collective_id=1, has_side_effects=True
        ),
        cost_estimate=pl.CostEstimate(
            flops=6 * 10**9, bytes_accessed=6 << 20, transcendentals=0
        ),
        name="fold",
    )(data, reply, flags, bins, *[jnp.asarray(table) for table in tables])


def on_device(voltages, antenna_gains, chirp_phase, offsets, flags, sample_phase_bins):
    shards, chans = (lax.axis_size("tm"), lax.axis_size("chan"))
    antennas, channels, samples = voltages.shape[1:]
    assert channels == 1 and shards >= 4 and shards & (shards - 1) == 0
    volts = voltages.reshape(2, antennas, samples // LANES, LANES)
    volts = jnp.transpose(volts, (0, 2, 1, 3)).reshape(2, samples // LANES * antennas, LANES)
    gains = jnp.transpose(antenna_gains, (0, 2, 1))
    data, reply = beam(volts, gains, offsets, chirp_phase.reshape(-1, LANES), shards)
    bins = sample_phase_bins.reshape(-1, LANES)
    dedispersed, small = fold(data, reply, flags, bins, chans, shards)
    lines = BINS // LANES // shards
    return (
        dedispersed.reshape(2, 1, HALF_ROWS * COLS),
        small[2 * lines : 2 * lines + 1, :WINDOWS],
        small[:lines].reshape(1, BINS // shards),
        small[lines : 2 * lines].reshape(BINS // shards),
    )


def solution(mesh):
    placed = (
        P(None, "tm", "chan", None),
        P(None, None, "chan"),
        P("chan", None),
        P("chan"),
        P("chan", "tm"),
        P("tm"),
    )
    return jax.shard_map(
        on_device,
        mesh=mesh,
        in_specs=placed,
        out_specs=(P(None, "chan", "tm"), P("chan", "tm"), P("chan", "tm"), P("tm")),
        check_vma=False,
    )
```

```python
import functools
import math

import jax
import jax.numpy as jnp
import numpy as np
from jax import lax
from jax.experimental import pallas as pl
from jax.experimental.pallas import tpu as pltpu
from jax.sharding import PartitionSpec as P

NFFT = 131072
OFFSET_BOUND = 4096
SKW = 1024
BINS = 2048


SK_WIDTH = 0.05
EPSILON = 1e-06

COLS = 1 << (NFFT.bit_length() - 1) // 2
ROWS = NFFT // COLS
HALF_ROWS = ROWS // 2
HALO_ROWS = OFFSET_BOUND // COLS
WIN_ROWS = SKW // COLS
WINDOWS = HALF_ROWS // WIN_ROWS
LOW_BINS = 32
HIGH_BINS = BINS // LOW_BINS
BLOCK_ROWS = 128
STEP_LINES = 8
LANES = 128
DEPTH = 256
PARTS = 4
PAIR_LAG = 1
CHIP_LAG = 2
PART_ROWS = HALF_ROWS // PARTS
MESH = pl.DeviceIdType.MESH


def bf16_split(table):
    high = table.astype(jnp.bfloat16)
    low = (table - high.astype(np.float32)).astype(jnp.bfloat16)
    return np.stack([high, low])


def unit_roots(turns, period):
    angle = -2.0 * math.pi / period * (turns % period)
    return (np.cos(angle).astype(np.float32), np.sin(angle).astype(np.float32))


def dft_table():
    index = np.arange(COLS, dtype=np.int64)
    real, imag = unit_roots(index[:, None] * index[None, :], COLS)
    return bf16_split(np.concatenate([-imag, real, imag]))


def twiddle():
    index = np.arange(HALF_ROWS, dtype=np.int64)
    rows = np.stack([2 * index, 2 * index + 1])
    return np.stack(unit_roots(rows[:, :, None] * np.arange(COLS, dtype=np.int64), NFFT))


def half_turns():
    index = np.arange(HALF_ROWS, dtype=np.int64)
    return np.stack(unit_roots(np.repeat(index[:, None], LANES, axis=1), ROWS))


def split(value):
    high = value.astype(jnp.bfloat16)
    return high, (value - high.astype(jnp.float32)).astype(jnp.bfloat16)


def product(*pairs):
    left, right = ([], [])
    for a, b in pairs:
        left += [a[0], a[0], a[1]]
        right += [b[0], b[1], b[0]]
    return jnp.dot(
        jnp.concatenate(left, axis=1),
        jnp.concatenate(right, axis=0),
        preferred_element_type=jnp.float32,
    )


def cos_sin(angle):
    half = 0.5 * angle
    square = half * half
    sine = jnp.full_like(square, 1.0 / math.factorial(13))
    for power in (11, 9, 7, 5, 3, 1):
        sine = sine * square + (-1.0) ** (power // 2) / math.factorial(power)
    sine = sine * half
    cosine = jnp.full_like(square, 1.0 / math.factorial(12))
    for power in (10, 8, 6, 4, 2, 0):
        cosine = cosine * square + (-1.0) ** (power // 2) / math.factorial(power)
    return 1.0 - 2.0 * sine * sine, 2.0 * sine * cosine


def response(phase, first, first_column, offset):
    index = first + lax.broadcasted_iota(jnp.int32, phase.shape, 0)
    column = first_column + lax.broadcasted_iota(jnp.int32, phase.shape, 1)
    index = index + ROWS * column
    turns = (index * offset) & (NFFT - 1)
    turns = jnp.where(turns >= NFFT // 2, turns - NFFT, turns)
    phase = phase + turns.astype(jnp.float32) * (2.0 * math.pi / NFFT)
    phase = jnp.where(phase > math.pi, phase - 2.0 * math.pi, phase)
    phase = jnp.where(phase < -math.pi, phase + 2.0 * math.pi, phase)
    return cos_sin(phase)


def weight_table(gains_ref, table_ref, antennas, me):
    total = gains_ref.shape[2]
    lane = lax.broadcasted_iota(jnp.int32, (8, LANES), 1)
    wide = []
    for part in range(2):
        row = gains_ref[part]
        if total < LANES:
            row = jnp.concatenate([row, jnp.zeros((1, LANES - total), jnp.float32)], axis=1)
        row = jnp.broadcast_to(row, (8, LANES))
        row = pltpu.roll(row, lax.rem(LANES - me * antennas, LANES), 1)
        row = jnp.where(lane < antennas, row, 0.0)
        width = antennas
        while width < LANES:
            row = row + pltpu.roll(row, width, 1)
            width *= 2
        wide.append(jnp.concatenate([row] * (DEPTH // LANES), axis=1)[:1])
    real, imag = wide
    half = DEPTH // antennas // 2
    shape = (half, DEPTH)
    tile = lax.broadcasted_iota(jnp.int32, shape, 1) // antennas
    index = lax.broadcasted_iota(jnp.int32, shape, 0)
    for source, pair in enumerate(((real, imag), (-imag, real))):
        for out, values in enumerate(pair):
            for parity in range(2):
                dense = jnp.where(tile == 2 * index + parity, values, 0.0)
                high, low = split(dense)
                at = (2 * out + parity) * half
                table_ref[source, at : at + half] = high
                table_ref[source, 4 * half + at : 4 * half + at + half] = low


def part_beam(table_ref, volt_ref, antennas, put):
    half = DEPTH // antennas // 2
    groups = volt_ref.shape[1] // DEPTH
    joined = 2 if groups % 2 == 0 else 1
    for at in range(groups // joined):
        total = None
        for source in range(2):
            lanes = [
                volt_ref[source, (joined * at + b) * DEPTH : (joined * at + b + 1) * DEPTH]
                for b in range(joined)
            ]
            right = lanes[0] if joined == 1 else jnp.concatenate(lanes, axis=1)
            term = jnp.dot(table_ref[source], right, preferred_element_type=jnp.float32)
            total = term if total is None else total + term
        total = total[: 4 * half] + total[4 * half :]
        for b in range(joined):
            block = total[:, b * LANES : (b + 1) * LANES]
            for out in range(2):
                even = block[2 * out * half : (2 * out + 1) * half]
                odd = block[(2 * out + 1) * half : (2 * out + 2) * half]
                put(out, (joined * at + b) * half, half, jnp.concatenate([even, odd], axis=1))


def beam_kernel(
    antennas, pairs, volt_ref, gains_hbm, offset_ref, chirp_hbm, turns_hbm, data_ref, response_ref,
    table_ref, vbuf, pair_send, pair_recv, chip_send, chip_recv, own_ref, halo_send, halo_ref,
    head_ref, gains_ref, chirp_ref, turns_ref, block_ref, load_sem, pair_sems, chip_sems, halo_sems,
    head_sems, side_sems,
):
    count = 2 * pairs
    me = lax.axis_index("tm")
    pair, core = (me // 2, lax.rem(me, 2))
    barrier = pltpu.get_barrier_semaphore()
    for step in range(1, count):
        pl.semaphore_signal(
            barrier, inc=1, device_id={"tm": lax.rem(me + step, count)}, device_id_type=MESH
        )
    size = vbuf.shape[3]

    levels = pairs.bit_length() - 1
    roles = range(pairs)
    halves = (range(1, pairs, 2), range(0, pairs, 2))

    def bit(level, side):
        return jnp.where(side == 0, 1 << level, 1 << (level + 1) % levels)

    def across(level, side):
        amount = bit(level, side)
        return amount * (1 - 2 * lax.rem(pair // amount, 2))

    def shard_of(role, other):
        side = 1 - core if other else core
        place = pair
        for level in range(levels):
            if role >> level & 1:
                place = place + across(level, side)
        return place * 2 + side

    def load(part, role, other):
        start = pl.multiple_of((shard_of(role, other) * PARTS + part) * size, size)
        slot = 2 * role + (0 if other else 1)
        return pltpu.make_async_copy(
            volt_ref.at[:, pl.ds(start, size)], vbuf.at[part, slot], load_sem.at[part, slot]
        )

    def begin(step, half):
        @pl.when(step < PARTS)
        def _():
            for role in halves[half]:
                load(step, role, True).start()

        @pl.when(step >= PAIR_LAG)
        def _():
            for role in halves[half]:
                load(step - PAIR_LAG, role, False).start()

        return 0

    gains_copy = pltpu.make_async_copy(gains_hbm, gains_ref, side_sems.at[2])
    gains_copy.start()
    for half in range(2):
        lax.fori_loop(0, PARTS + PAIR_LAG, lambda step, carry, half=half: begin(step, half), 0)
    side = [
        pltpu.make_async_copy(chirp_hbm, chirp_ref, side_sems.at[0]),
        pltpu.make_async_copy(turns_hbm, turns_ref, side_sems.at[1]),
    ]
    for copy in side:
        copy.start()
    gains_copy.wait()
    weight_table(gains_ref, table_ref, antennas, me)

    def place_of(role):
        return role // 2 + (0 if role % 2 else pairs // 2)

    def pair_copy(part, half):
        slots = slice(half * (pairs // 2), (half + 1) * (pairs // 2))
        return pltpu.make_async_remote_copy(
            src_ref=pair_send.at[part, slots], dst_ref=pair_recv.at[part, slots],
            send_sem=pair_sems.at[0, part, half], recv_sem=pair_sems.at[1, part, half],
            device_id={"tm": pair * 2 + (1 - core)}, device_id_type=MESH,
        )

    def level_of(role):
        return (role & -role).bit_length() - 1

    def first_slot(level):
        return pairs - (pairs >> level)

    def slot_of(role):
        level = level_of(role)
        return first_slot(level) + (role >> (level + 1))

    def chip_copy(part, level):
        slots = slice(first_slot(level), first_slot(level + 1))
        return pltpu.make_async_remote_copy(
            src_ref=chip_send.at[part, slots], dst_ref=chip_recv.at[part, slots],
            send_sem=chip_sems.at[0, part, level], recv_sem=chip_sems.at[1, part, level],
            device_id={"tm": (pair + across(level, core)) * 2 + core}, device_id_type=MESH,
        )

    def halo_copy(part):
        return pltpu.make_async_remote_copy(
            src_ref=halo_send.at[part], dst_ref=halo_ref.at[part],
            send_sem=halo_sems.at[0, part], recv_sem=halo_sems.at[1, part],
            device_id={"tm": lax.rem(me + 1, count)}, device_id_type=MESH,
        )

    def head_copy():
        return pltpu.make_async_remote_copy(
            src_ref=halo_send.at[0, :, 0:HALO_ROWS], dst_ref=head_ref,
            send_sem=head_sems.at[0], recv_sem=head_sems.at[1],
            device_id={"tm": lax.rem(me + count - 1, count)}, device_id_type=MESH,
        )

    def pass_on(part, level):
        chip_copy(part, level).wait_recv()
        for role in roles:
            if role & ((2 << level) - 1) == 0:
                arrived = chip_recv[part, slot_of(role + (1 << level))].astype(jnp.float32)
                total = own_ref[part, role // 2] + arrived
                if role and level_of(role) == level + 1:
                    chip_send[part, slot_of(role)] = total.astype(jnp.bfloat16)
                else:
                    own_ref[part, role // 2] = total
                    if role == 0 and level == levels - 1:
                        halo_send[part] = total.astype(jnp.bfloat16)
        if level < levels - 1:
            chip_copy(part, level + 1).start()

    def finish(part):
        pass_on(part, levels - 1)

        @pl.when(me < count - 1)
        def _():
            halo_copy(part).start()

    def chirp_block(at):
        stride = ROWS // LANES
        for half in range(COLS // LANES):
            columns = chirp_ref[
                pl.ds(at + half * LANES * stride, LANES, stride=stride), :
            ]
            phase = jnp.transpose(columns, (1, 0))
            for out, value in enumerate(response(phase, at * LANES, half * LANES, offset)):
                block_ref[...] = value * (1.0 / NFFT)
                for parity in range(2):
                    rows = pl.ds(pl.multiple_of(at * (LANES // 2), LANES // 2), LANES // 2)
                    response_ref[out, parity, rows, half * LANES : (half + 1) * LANES] = (
                        block_ref[pl.ds(parity, LANES // 2, stride=2), :]
                    )

    def combine(part, first=None):
        rows = slice(part * PART_ROWS, (part + 1) * PART_ROWS)
        before = [halo_ref[part, out].astype(jnp.float32) for out in range(2)]
        if first is not None:
            before = [
                jnp.concatenate([head, value[HALO_ROWS:]], axis=0)
                for head, value in zip(first, before)
            ]
        after = [own_ref[part, 0, 0], own_ref[part, 0, 1]]
        real, imag = (before[0] - after[0], before[1] - after[1])
        cosine, sine = [
            jnp.concatenate([turns_ref[out, rows]] * (COLS // LANES), axis=1) for out in range(2)
        ]
        both = (
            (before[0] + after[0], before[1] + after[1]),
            (real * cosine - imag * sine, real * sine + imag * cosine),
        )
        for kind, values in enumerate(both):
            for out, value in enumerate(values):
                data_ref[kind, out, 0, rows], data_ref[kind, out, 1, rows] = split(value)

    def give(part, half):
        for role in halves[half]:
            load(part, role, True).wait()
        for role in halves[half]:

            def put(out, at, rows, value, role=role):
                pair_send[part, place_of(role), out, at : at + rows] = value

            part_beam(table_ref, vbuf.at[part, 2 * role], antennas, put)
        if half == 0:

            @pl.when(part == 0)
            def _():
                pl.semaphore_wait(barrier, count - 1)

        pair_copy(part, half).start()

    def take(part, half):
        for role in halves[half]:
            load(part, role, False).wait()
        pair_copy(part, half).wait_recv()
        for role in halves[half]:

            def put(out, at, rows, value, role=role):
                value = value + pair_recv[part, place_of(role), out, at : at + rows]
                if role % 2:
                    chip_send[part, slot_of(role), out, at : at + rows] = value.astype(jnp.bfloat16)
                else:
                    own_ref[part, role // 2, out, at : at + rows] = value

            part_beam(table_ref, vbuf.at[part, 2 * role + 1], antennas, put)
        if half == 0:
            chip_copy(part, 0).start()

    def run(step, half):
        @pl.when(step < PARTS)
        def _():
            give(step, half)

        @pl.when((step >= PAIR_LAG) & (step < PARTS + PAIR_LAG))
        def _():
            take(step - PAIR_LAG, half)

    def spread(step, carry):
        run(step, 0)
        return carry

    def gather(step, carry):
        run(step, 1)

        @pl.when(step >= CHIP_LAG)
        def _():
            for level in range(levels - 1):
                pass_on(step - CHIP_LAG, level)

        return carry

    lax.fori_loop(0, PARTS + PAIR_LAG, spread, 0)
    lax.fori_loop(0, PARTS + CHIP_LAG, gather, 0)
    for copy in side:
        copy.wait()
    offset = offset_ref[0]

    def settle(step, carry):
        finish(step)

        @pl.when((step == 0) & (me > 0))
        def _():
            head_copy().start()

        @pl.when(step < ROWS // LANES)
        def _():
            chirp_block(step)

        return carry

    lax.fori_loop(0, PARTS, settle, 0)

    @pl.when(me == 0)
    def _():
        halo_ref[...] = jnp.zeros((PARTS, 2, PART_ROWS, COLS), jnp.bfloat16)

    @pl.when(me == count - 1)
    def _():
        head_ref[...] = jnp.zeros((2, HALO_ROWS, COLS), jnp.bfloat16)

    for part in range(PARTS):

        @pl.when(me > 0)
        def _():
            halo_copy(part).wait_recv()

        first = None
        if part == 0:

            @pl.when(me < count - 1)
            def _():
                head_copy().wait_recv()

            spot = lax.broadcasted_iota(jnp.int32, (HALO_ROWS, COLS), 0) * COLS
            spot = spot + lax.broadcasted_iota(jnp.int32, (HALO_ROWS, COLS), 1)
            first = [
                jnp.where(
                    spot < offset,
                    head_ref[out].astype(jnp.float32),
                    halo_ref[0, out, 0:HALO_ROWS].astype(jnp.float32),
                )
                for out in range(2)
            ]
        combine(part, first)

    @pl.when(me > 0)
    def _():
        head_copy().wait_send()

    @pl.when(me < count - 1)
    def _():
        for part in range(PARTS):
            halo_copy(part).wait_send()

    def drain(part, carry):
        for half in range(2):
            pair_copy(part, half).wait_send()
        for level in range(levels):
            chip_copy(part, level).wait_send()
        return carry

    lax.fori_loop(0, PARTS, drain, 0)


def beam(volts, gains, offset, chirp, shards):
    pairs = shards // 2
    size = volts.shape[1] // shards // PARTS
    antennas = size * LANES // (PART_ROWS * COLS)
    half = DEPTH // antennas // 2
    block = (2, PART_ROWS, COLS)
    vmem = pl.BlockSpec(memory_space=pltpu.VMEM)
    hbm = pl.BlockSpec(memory_space=pltpu.HBM)
    keep = functools.partial(pltpu.with_memory_space_constraint, memory_space=pltpu.HBM)
    return pl.pallas_call(
        functools.partial(beam_kernel, antennas, pairs),
        out_shape=(
            jax.ShapeDtypeStruct((2, 2, 2, HALF_ROWS, COLS), jnp.bfloat16),
            jax.ShapeDtypeStruct((2, 2, HALF_ROWS, COLS), jnp.float32),
        ),
        in_specs=[hbm, hbm, pl.BlockSpec(memory_space=pltpu.SMEM), hbm, hbm],
        out_specs=(vmem, vmem),
        scratch_shapes=[
            pltpu.VMEM((2, 8 * half, DEPTH), jnp.bfloat16),
            pltpu.VMEM((PARTS, shards, 2, size, LANES), jnp.bfloat16),
            pltpu.VMEM((PARTS, pairs) + block, jnp.float32),
            pltpu.VMEM((PARTS, pairs) + block, jnp.float32),
            pltpu.VMEM((PARTS, pairs - 1) + block, jnp.bfloat16),
            pltpu.VMEM((PARTS, pairs - 1) + block, jnp.bfloat16),
            pltpu.VMEM((PARTS, pairs // 2) + block, jnp.float32),
            pltpu.VMEM((PARTS,) + block, jnp.bfloat16),
            pltpu.VMEM((PARTS,) + block, jnp.bfloat16),
            pltpu.VMEM((2, HALO_ROWS, COLS), jnp.bfloat16),
            pltpu.VMEM(gains.shape, jnp.float32),
            pltpu.VMEM((NFFT // LANES, LANES), jnp.float32),
            pltpu.VMEM((2, HALF_ROWS, LANES), jnp.float32),
            pltpu.VMEM((LANES, LANES), jnp.float32),
            pltpu.SemaphoreType.DMA((PARTS, shards)),
            pltpu.SemaphoreType.DMA((2, PARTS, 2)),
            pltpu.SemaphoreType.DMA((2, PARTS, pairs.bit_length() - 1)),
            pltpu.SemaphoreType.DMA((2, PARTS)),
            pltpu.SemaphoreType.DMA((2,)),
            pltpu.SemaphoreType.DMA((3,)),
        ],
        compiler_params=pltpu.CompilerParams(
            vmem_limit_bytes=44 << 20, collective_id=0, has_side_effects=True
        ),
        cost_estimate=pl.CostEstimate(
            flops=3 * 10**9, bytes_accessed=18 << 20, transcendentals=0
        ),
        name="beam",
    )(keep(volts), keep(gains), offset, keep(chirp), keep(jnp.asarray(half_turns())))


def spectrum_kernel(
    data_ref, response_ref, flags_ref, dft_ref, twist_ref, turns_ref, dedispersed_ref, weight_ref,
    weighted_ref, blend_ref,
):
    def table(start, count=1):
        rows = slice(start * COLS, (start + count) * COLS)
        return (dft_ref[0, rows], dft_ref[1, rows])

    minus_table, real_table, imag_table = (table(0), table(1), table(2))
    forward, cross = (table(1, 2), table(0, 2))
    pairs = []
    for kind in range(2):
        given = [(data_ref[kind, out, 0], data_ref[kind, out, 1]) for out in range(2)]
        both = product((forward, given[0]), (cross, given[1]))
        pairs.append((both[:HALF_ROWS], both[HALF_ROWS:]))
    for kind in range(2):
        real, imag = pairs[kind]
        cosine, sine = (twist_ref[0, kind], twist_ref[1, kind])
        pairs[kind] = (split(real * cosine - imag * sine), split(real * sine + imag * cosine))
    for kind in range(2):
        real, imag = pairs[kind]
        pairs[kind] = (
            product((real, real_table), (imag, minus_table)),
            product((real, imag_table), (imag, real_table)),
        )
    for kind in range(2):
        real, imag = pairs[kind]
        turn, tilt = (response_ref[0, kind], response_ref[1, kind])
        pairs[kind] = (split(real * turn - imag * tilt), split(real * tilt + imag * turn))
    for kind in range(2):
        real, imag = pairs[kind]
        pairs[kind] = (
            product((real, real_table), (imag, imag_table)),
            product((real, minus_table), (imag, real_table)),
        )
    for kind in range(2):
        real, imag = pairs[kind]
        cosine, sine = (twist_ref[0, kind], twist_ref[1, kind])
        pairs[kind] = (split(real * cosine + imag * sine), split(imag * cosine - real * sine))
    for kind in range(2):
        real, imag = pairs[kind]
        both = product((cross, real), (forward, imag))
        pairs[kind] = (both[HALF_ROWS:], both[:HALF_ROWS])

    flag = flags_ref[...]
    if WINDOWS < LANES:
        flag = jnp.concatenate([flag, jnp.zeros((1, LANES - WINDOWS), jnp.int32)], axis=1)
    keep_row = (1 - flag).astype(jnp.float32)
    shape = (BLOCK_ROWS, LANES)
    row_index = lax.broadcasted_iota(jnp.int32, shape, 0)
    lane_index = lax.broadcasted_iota(jnp.int32, shape, 1)

    def window_sum(values):
        total = jnp.broadcast_to(jnp.sum(values, axis=1, keepdims=True), shape)
        reach = 1
        while reach < WIN_ROWS:
            up, down = (pltpu.roll(total, BLOCK_ROWS - reach, 0), pltpu.roll(total, reach, 0))
            total = total + jnp.where(row_index % (2 * reach) < reach, up, down)
            reach *= 2
        return total

    per_line = COLS // LANES
    weight_row = jnp.zeros((1, LANES), jnp.float32)
    for start in range(0, HALF_ROWS, BLOCK_ROWS):
        rows = slice(start, start + BLOCK_ROWS)
        cosine, sine = [
            jnp.concatenate([turns_ref[out, rows]] * (COLS // LANES), axis=1) for out in range(2)
        ]
        (real, imag), (odd_real, odd_imag) = [[value[rows] for value in pair] for pair in pairs]
        real = real - (odd_real * cosine + odd_imag * sine)
        imag = imag - (odd_imag * cosine - odd_real * sine)
        for out, value in enumerate((real, imag)):
            for at in range(per_line):
                places = pl.ds(2 * at + out, BLOCK_ROWS, stride=2 * per_line)
                blend_ref[places, :] = value[:, at * LANES : (at + 1) * LANES]
        lines = 2 * per_line * BLOCK_ROWS
        dedispersed_ref[start * 2 * per_line : start * 2 * per_line + lines] = blend_ref[
            ...
        ].astype(jnp.bfloat16)
        power = real * real + imag * imag
        first_sum, second_sum = (window_sum(power), window_sum(power * power))
        kurtosis = (
            (SKW + 1.0)
            / (SKW - 1.0)
            * (SKW * second_sum / (first_sum * first_sum + EPSILON) - 1.0)
        )
        scaled = (kurtosis - 1.0) / SK_WIDTH
        window = (row_index + start) // WIN_ROWS
        keep = jnp.where(lane_index == window, jnp.broadcast_to(keep_row, shape), 0.0)
        keep = jnp.sum(keep, axis=1, keepdims=True)
        sk_weight = keep / (1.0 + scaled * scaled)
        chosen = (row_index + start) == lane_index * WIN_ROWS
        weight_row = weight_row + jnp.sum(
            jnp.where(chosen, sk_weight, 0.0), axis=0, keepdims=True
        )
        for at in range(COLS // LANES):
            lanes = slice(at * LANES, (at + 1) * LANES)
            value = (sk_weight * power[:, lanes]).astype(jnp.bfloat16)
            places = pl.ds(start * per_line + at, BLOCK_ROWS, stride=per_line)
            weighted_ref[places, :] = value.astype(jnp.float32)

    weight_ref[...] = weight_row[:, :WINDOWS]


def fold_kernel(
    chans, shards, weighted_ref, bins_ref, small_ref, high_ref, low_ref, send_ref, recv_ref, sems
):
    everyone = chans * shards
    mine = lax.axis_index("chan")
    here = mine * shards + lax.axis_index("tm")
    barrier = pltpu.get_barrier_semaphore()

    def target(index):
        return {"chan": index // shards, "tm": lax.rem(index, shards)}

    def greet(step, carry):
        pl.semaphore_signal(
            barrier, inc=1, device_id=target(lax.rem(here + step, everyone)), device_id_type=MESH
        )
        return carry

    lax.fori_loop(1, everyone, greet, 0)
    per_line = COLS // LANES
    bins = bins_ref[...]
    shift = LOW_BINS.bit_length() - 1
    high_ref[...] = lax.shift_right_logical(bins, jnp.full_like(bins, shift)).astype(jnp.float32)
    low_ref[...] = (bins & (LOW_BINS - 1)).astype(jnp.float32)
    high_index = lax.broadcasted_iota(jnp.int32, (HIGH_BINS, LANES), 0)
    high_index = high_index.astype(jnp.float32).astype(jnp.bfloat16)
    low_index = lax.broadcasted_iota(jnp.int32, (LOW_BINS, LANES), 0)
    low_index = low_index.astype(jnp.float32).astype(jnp.bfloat16)
    minus, zero = (jnp.bfloat16(-1.0), jnp.bfloat16(0.0))

    def step(at, total):
        start = at * STEP_LINES
        left, right = ([], [])

        def spread(block, line, count):
            return jnp.broadcast_to(block[line : line + 1], (count, LANES)).astype(jnp.bfloat16)

        lines_here = pl.ds(start, STEP_LINES)
        highs, lows, values = (high_ref[lines_here], low_ref[lines_here], weighted_ref[lines_here])
        for line in range(STEP_LINES):
            left.append(jnp.where(high_index == spread(highs, line, HIGH_BINS), minus, zero))
            value = spread(values, line, LOW_BINS)
            right.append(jnp.where(low_index == spread(lows, line, LOW_BINS), value, zero))
        return total - lax.dot_general(
            jnp.concatenate(left, axis=1),
            jnp.concatenate(right, axis=1),
            ((((1,), (1,))), ((), ())),
            preferred_element_type=jnp.float32,
        )

    totals = [jnp.zeros((HIGH_BINS, LOW_BINS), jnp.float32)] * 2
    for at in range(HALF_ROWS * per_line // STEP_LINES):
        totals[at % 2] = step(at, totals[at % 2])
    total = totals[0] + totals[1]
    per_row = LANES // LOW_BINS
    total = jnp.concatenate([total, jnp.zeros((HIGH_BINS, LANES - LOW_BINS), jnp.float32)], axis=1)
    place = lax.broadcasted_iota(jnp.int32, (HIGH_BINS, LANES), 0) % per_row
    moved = jnp.where(place == 0, total, 0.0)
    for at in range(1, per_row):
        moved = moved + jnp.where(place == at, pltpu.roll(total, at * LOW_BINS, 1), 0.0)
    lines = BINS // LANES // shards
    for line in range(BINS // LANES):
        send_ref[line // lines, line % lines : line % lines + 1] = jnp.sum(
            moved[line * per_row : (line + 1) * per_row], axis=0, keepdims=True
        )
    pl.semaphore_wait(barrier, everyone - 1)

    def outgoing(index):
        return pltpu.make_async_remote_copy(
            src_ref=send_ref.at[lax.rem(index, shards)], dst_ref=recv_ref.at[here],
            send_sem=sems.at[0, index], recv_sem=sems.at[1, here],
            device_id=target(index), device_id_type=MESH,
        )

    def incoming(index):
        return pltpu.make_async_remote_copy(
            src_ref=send_ref.at[lax.rem(index, shards)], dst_ref=recv_ref.at[index],
            send_sem=sems.at[0, index], recv_sem=sems.at[1, index],
            device_id=target(index), device_id_type=MESH,
        )

    def begin(step, carry):
        outgoing(lax.rem(here + step, everyone)).start()
        return carry

    def arrive(step, carry):
        incoming(lax.rem(here + everyone - step, everyone)).wait_recv()
        return carry

    def leave(step, carry):
        outgoing(lax.rem(here + step, everyone)).wait_send()
        return carry

    lax.fori_loop(1, everyone, begin, 0)
    recv_ref[here] = send_ref[lax.axis_index("tm")]
    lax.fori_loop(1, everyone, arrive, 0)
    scale = BINS / (HALF_ROWS * COLS * shards)
    band = None
    for chan in range(chans):
        line = recv_ref[chan * shards]
        for at in range(1, shards):
            line = line + recv_ref[chan * shards + at]
        line = line * scale
        own = jnp.where(mine == chan, line, 0.0)
        band, profile = (line, own) if band is None else (band + line, profile + own)
    small_ref[0:lines] = profile
    small_ref[lines : 2 * lines] = band
    lax.fori_loop(1, everyone, leave, 0)


def spectrum(data, reply, flags):
    vmem = pl.BlockSpec(memory_space=pltpu.VMEM)
    tables = (dft_table(), twiddle(), half_turns())
    lines = HALF_ROWS * COLS // LANES
    return pl.pallas_call(
        spectrum_kernel,
        out_shape=(
            jax.ShapeDtypeStruct((2 * lines, LANES), jnp.bfloat16),
            jax.ShapeDtypeStruct((1, WINDOWS), jnp.float32),
            jax.ShapeDtypeStruct((lines, LANES), jnp.float32),
        ),
        in_specs=[vmem] * 6,
        out_specs=(vmem,) * 3,
        scratch_shapes=[pltpu.VMEM((2 * BLOCK_ROWS * COLS // LANES, LANES), jnp.float32)],
        compiler_params=pltpu.CompilerParams(vmem_limit_bytes=40 << 20),
        cost_estimate=pl.CostEstimate(
            flops=5 * 10**9, bytes_accessed=6 << 20, transcendentals=0
        ),
        name="spectrum",
    )(data, reply, flags, *[jnp.asarray(table) for table in tables])


def fold(weighted, bins, chans, shards):
    vmem = pl.BlockSpec(memory_space=pltpu.VMEM)
    lines = BINS // LANES // shards
    return pl.pallas_call(
        functools.partial(fold_kernel, chans, shards),
        out_shape=jax.ShapeDtypeStruct((2 * lines, LANES), jnp.float32),
        in_specs=[vmem, vmem],
        out_specs=vmem,
        scratch_shapes=[
            pltpu.VMEM(bins.shape, jnp.float32),
            pltpu.VMEM(bins.shape, jnp.float32),
            pltpu.VMEM((shards, lines, LANES), jnp.float32),
            pltpu.VMEM((chans * shards, lines, LANES), jnp.float32),
            pltpu.SemaphoreType.DMA((2, chans * shards)),
        ],
        compiler_params=pltpu.CompilerParams(
            vmem_limit_bytes=16 << 20, collective_id=1, has_side_effects=True
        ),
        cost_estimate=pl.CostEstimate(flops=10**9, bytes_accessed=1 << 20, transcendentals=0),
        name="fold",
    )(weighted, bins)


def on_device(voltages, antenna_gains, chirp_phase, offsets, flags, sample_phase_bins):
    shards, chans = (lax.axis_size("tm"), lax.axis_size("chan"))
    antennas, channels, samples = voltages.shape[1:]
    assert channels == 1 and shards >= 4 and shards & (shards - 1) == 0
    volts = voltages.reshape(2, antennas, samples // LANES, LANES)
    volts = jnp.transpose(volts, (0, 2, 1, 3)).reshape(2, samples // LANES * antennas, LANES)
    gains = jnp.transpose(antenna_gains, (0, 2, 1))
    data, reply = beam(volts, gains, offsets, chirp_phase.reshape(-1, LANES), shards)
    bins = sample_phase_bins.reshape(-1, LANES)
    dedispersed, weight, weighted = spectrum(data, reply, flags)
    small = fold(weighted, bins, chans, shards)
    lines = BINS // LANES // shards
    dedispersed = jnp.transpose(dedispersed.reshape(-1, 2, LANES), (1, 0, 2))
    return (
        dedispersed.reshape(2, 1, HALF_ROWS * COLS),
        weight,
        small[:lines].reshape(1, BINS // shards),
        small[lines:].reshape(BINS // shards),
    )


def solution(mesh):
    placed = (
        P(None, "tm", "chan", None),
        P(None, None, "chan"),
        P("chan", None),
        P("chan"),
        P("chan", "tm"),
        P("tm"),
    )
    return jax.shard_map(
        on_device,
        mesh=mesh,
        in_specs=placed,
        out_specs=(P(None, "chan", "tm"), P("chan", "tm"), P("chan", "tm"), P("tm")),
        check_vma=False,
    )
```
